512 devices in a mesh: fsdp: 128 (over y, z, core), dp: 4 (over x).
Axes of the slice: x: 4, y: 8, z: 8, core: 2. Of those that a mesh axis runs over, the one named last changes fastest.
Arguments:
- tokens: bfloat16 [512, 4096], P('dp', 'fsdp'), may hold values from -6 to 6
- out_grad: bfloat16 [512, 5120], P('dp', 'fsdp'), may hold values from -0.26367188 to 0.26367188
- master: float32 [4096, 5120], P('fsdp'), may hold values from -0.09375 to 0.09375
- moment_one: float32 [4096, 5120], P('fsdp'), may hold values from -3 to 3
- moment_two: float32 [4096, 5120], P('fsdp'), may hold values from 0.1 to 4
- flags: int32 [512, 16], P(('fsdp', 'dp')), may hold values 0 or 1
- steps: int32 [16], replicated, may hold values from 1 to 8
- rate: float32 [1], replicated, may hold values from 0.001 to 0.01
Outputs:
- master_next: float32 [4096, 5120], P('fsdp')
- moment_one_next: float32 [4096, 5120], P('fsdp')
- moment_two_next: float32 [4096, 5120], P('fsdp')
- weight_half: bfloat16 [4096, 5120], P('fsdp')
- steps_next: int32 [16], replicated
- outputs: bfloat16 [512, 5120], P('dp', 'fsdp')
The draws below stay inside these ranges and needn't reach their ends.
All inputs are finite; a program needn't handle non-finite values. No bound on the sum of `flags` on one device may be relied on, other than what follows from the above.
Results may differ from the reference program's by a relative error of at most 0.0049.
Values may be sent and summed in bfloat16 or wider, within the bound.
No kernel may reach another device: no remote copies, remote signals or barrier semaphores. Data moves between devices by JAX's collectives and lax.ppermute only.
A program may use at most 64 MiB of HBM per device.

```python
import math
import jax
import jax.numpy as jnp
from jax import lax

D = 4096
R = 5120
BUCKETS = 16
TOK_G = 128
TOKENS = 512
N_FSDP = 128
N_DP = 4


def touch_ends(values, key, smallest, high):
    extent = values.shape
    place = [jax.random.randint(jax.random.fold_in(key, axis), (), 0, extent[axis]) for axis in range(len(extent))]
    values = values.at[tuple(place)].set(smallest)
    longest = extent.index(max(extent))
    place[longest] = (place[longest] + 1) % extent[longest]
    return values.at[tuple(place)].set(high)


def block_scale(rng, extent, cuts, smallest, largest):
    loudness, own = 1.0, jax.random.fold_in(rng, 6)
    for position, shards_of in cuts:
        heights = jnp.exp(jax.random.uniform(jax.random.fold_in(own, position), (shards_of,), jnp.float32, smallest / len(cuts), largest / len(cuts)))
        loudness = loudness * jnp.repeat(heights, extent[position] // shards_of).reshape([-1 if axis == position else 1 for axis in range(len(extent))])
    return loudness


def normal_values(stream_key, dims, spread, limit, cuts=(), kind=jnp.bfloat16):
    values = jax.random.normal(stream_key, dims, jnp.float32) * spread
    if len(cuts) > 0:
        values = block_scale(stream_key, dims, cuts, -0.22, 0.18) * values
    return jnp.clip(values, min=-limit, max=limit).astype(kind)


def setup_inputs(seed: int = 0) -> dict:
    streams_of = jax.random.split(jax.random.key(seed), 9)
    return {
        "tokens": normal_values(streams_of[0], (TOKENS, D), 1.0, 6.0, ((0, 4), (1, 128))),
        "out_grad": normal_values(streams_of[1], (TOKENS, R), (1.0 / (TOK_G * N_DP) ** 0.5), 0.26367188, ((0, 4), (1, 128))),
        "master": normal_values(streams_of[2], (D, R), D ** -0.5, 0.09375, ((0, 128),), jnp.float32),
        "moment_one": normal_values(streams_of[3], (D, R), 0.5, 3.0, ((0, 128),), jnp.float32),
        "moment_two": jnp.clip(jnp.exp(math.log(4.0) - 3.6888794 * jax.random.uniform(streams_of[4], (D, R), jnp.float32) ** block_scale(streams_of[4], (D, R), ((0, 128),), -0.2, 0.2)), 0.1, 4.0),
        "flags": touch_ends((jax.random.randint(streams_of[5], (N_FSDP * N_DP, BUCKETS), 0, N_FSDP * N_DP * 3 // 2) < 1).astype(jnp.int32), jax.random.fold_in(streams_of[5], 1), 0, 1),
        "steps": touch_ends(jax.random.randint(streams_of[6], (BUCKETS,), 1, 9), jax.random.fold_in(streams_of[6], 1), 1, 8).astype(jnp.int32),
        "rate": jnp.clip(jnp.exp(jax.random.uniform(streams_of[7], (1,), jnp.float32, math.log(0.001), math.log(0.01))), 0.001, 0.01),
    }


first_decay = 0.9
second_decay = 0.95
epsilon = 1e-08

def reference(tokens, out_grad, master, moment_one, moment_two, flags, steps, rate):
    gradient = lax.dot_general(tokens, out_grad, (((0,), (0,)), ((), ())), preferred_element_type=jnp.float32)
    bucket_width = master.shape[1] // BUCKETS
    counts = lax.optimization_barrier(jnp.sum(flags, axis=0)).astype(jnp.int32)
    commit_bucket = counts == 0
    commit = jnp.repeat(commit_bucket, bucket_width)[None, :]
    times = jnp.repeat(steps + 1, bucket_width).astype(jnp.float32)[None, :]
    first = first_decay * moment_one + (1.0 - first_decay) * gradient
    second = second_decay * moment_two + (1.0 - second_decay) * gradient * gradient
    fix_one = 1.0 - jnp.power(jnp.float32(first_decay), times)
    fix_two = 1.0 - jnp.power(jnp.float32(second_decay), times)
    candidate = master - rate[0] * (first / fix_one) / (jnp.sqrt(second / fix_two) + epsilon)
    master_next = jnp.where(commit, candidate, master)
    moment_one_next = jnp.where(commit, first, moment_one)
    moment_two_next = jnp.where(commit, second, moment_two)
    weight_half = master_next.astype(jnp.bfloat16)
    steps_next = steps + commit_bucket.astype(jnp.int32)
    outputs = jnp.dot(tokens, weight_half, preferred_element_type=jnp.float32).astype(jnp.bfloat16)
    return (master_next, moment_one_next, moment_two_next, weight_half, steps_next, outputs)
```

```python
import jax
import jax.numpy as jnp
from jax import lax
from jax.sharding import Mesh
from jax.sharding import PartitionSpec as P

BUCKETS = 16
FSDP = ("y", "zh", "zl", "c")
ALL = FSDP + ("x",)
ZC = ("zh", "zl", "c")
XY = ("x", "y")
NX, NY, NZC = 4, 8, 16
first_decay = 0.9
second_decay = 0.95
epsilon = 1e-08
bf16, f32 = jnp.bfloat16, jnp.float32


def exchange(x, axes):
    return lax.all_to_all(x, axes, 0, 0, tiled=True)


def everyone(x, axes, n):
    return exchange(jnp.broadcast_to(x[None], (n, *x.shape)), axes)


def adam(master, one, two, gradient, commit, times, rate):
    first = first_decay * one + (1.0 - first_decay) * gradient
    second = second_decay * two + (1.0 - second_decay) * gradient * gradient
    fix_one = 1.0 - jnp.power(f32(first_decay), times)
    fix_two = 1.0 - jnp.power(f32(second_decay), times)
    candidate = master - rate * (first / fix_one) / (jnp.sqrt(second / fix_two) + epsilon)
    return (
        jnp.where(commit, candidate, master),
        jnp.where(commit, first, one),
        jnp.where(commit, second, two),
    )


def local(tokens, out_grad, master, moment_one, moment_two, flags, steps, rate):
    rows, width = master.shape
    bucket_width = width // BUCKETS
    tok_g, chunk = out_grad.shape
    cols = chunk * NZC // NX
    ix, iy = lax.axis_index("x"), lax.axis_index("y")
    lanes = 128

    mine = jnp.pad(flags.astype(bf16), ((0, 7), (0, lanes - BUCKETS)))
    seen = jnp.max(everyone(mine, XY, NX * NY), axis=0)

    tok = everyone(tokens.T, XY, NX * NY).reshape(NX, NY * rows, tok_g)

    perm = [(zh * NX + x, x * NX + zh) for zh in range(NX) for x in range(NX)]
    og = lax.ppermute(out_grad.T, ("zh", "x"), perm)
    og = everyone(jnp.concatenate([og, seen], axis=0), ZC, NZC)
    counts = jnp.max(og[:, chunk, :BUCKETS], axis=0)
    og = og[:, :chunk].reshape(NX, cols, tok_g)
    commit_bucket = counts == 0

    def block(p):
        q = lax.dynamic_index_in_dim(p.reshape(rows, NY, NX, cols), ix, 2, keepdims=False)
        return q.transpose(1, 0, 2)

    high = master.astype(bf16)
    low = (master - high.astype(f32)).astype(bf16)
    params = jnp.concatenate(
        [block(high), block(low), block(moment_one.astype(bf16)), block(moment_two.astype(bf16))], axis=2
    )
    params = exchange(params, "y").reshape(NY * rows, 4 * cols).astype(f32)
    b_master = params[:, :cols] + params[:, cols : 2 * cols]
    b_one = params[:, 2 * cols : 3 * cols]
    b_two = params[:, 3 * cols :]

    grad = sum(
        lax.dot_general(tok[k], og[k], (((1,), (1,)), ((), ())), preferred_element_type=f32) for k in range(NX)
    )
    send = jnp.broadcast_to(grad.astype(bf16).reshape(1, NY, rows, cols), (NX, NY, rows, cols))
    full = exchange(send.reshape(NX * NY, rows, cols), XY)
    full = full.reshape(NX, NY, rows, cols).transpose(2, 1, 0, 3).reshape(rows, width).astype(f32)

    bucket = (iy * NX + ix) * cols // bucket_width
    b_times = (steps[bucket] + 1).astype(f32)
    half, _, _ = adam(b_master, b_one, b_two, grad, commit_bucket[bucket], b_times, rate[0])
    half = half.astype(bf16)
    part = lax.dot_general(
        tok, half, (((1,), (0,)), ((), ())), preferred_element_type=f32
    )
    part = part.transpose(0, 2, 1).reshape(NZC, chunk, tok_g)
    total = jnp.sum(exchange(part, ZC), axis=0)
    result = lax.ppermute(total.astype(bf16), ("zh", "x"), perm).T

    commit = jnp.repeat(commit_bucket, bucket_width)[None, :]
    times = jnp.repeat(steps + 1, bucket_width).astype(f32)[None, :]
    master_next, one_next, two_next = adam(master, moment_one, moment_two, full, commit, times, rate[0])
    steps_next = steps + commit_bucket.astype(jnp.int32)
    return master_next, one_next, two_next, master_next.astype(bf16), steps_next, result


def solution(mesh):
    split = Mesh(mesh.devices.reshape(8, 4, 2, 2, 4), ALL)
    in_specs = (P("x", FSDP), P("x", FSDP), P(FSDP), P(FSDP), P(FSDP), P(ALL), P(), P())
    out_specs = (P(FSDP), P(FSDP), P(FSDP), P(FSDP), P(), P("x", FSDP))
    return jax.shard_map(local, mesh=split, in_specs=in_specs, out_specs=out_specs, check_vma=False)
```

```python
import jax
import jax.numpy as jnp
from jax import lax
from jax.experimental import pallas as pl
from jax.experimental.pallas import tpu as pltpu
from jax.sharding import Mesh
from jax.sharding import PartitionSpec as P

BUCKETS = 16
FSDP = ("y", "zh", "zl", "c")
ALL = FSDP + ("x",)
ZC = ("zh", "zl", "c")
XY = ("x", "y")
NX, NY, NZC = 4, 8, 16
LANES = 128
first_decay = 0.9
second_decay = 0.95
epsilon = 1e-08
bf16, f32 = jnp.bfloat16, jnp.float32
VMEM, SMEM = pltpu.VMEM, pltpu.SMEM
SMALL = pltpu.CompilerParams(vmem_limit_bytes=16 * 1024 * 1024)


def exchange(x, axes):
    return lax.all_to_all(x, axes, 0, 0, tiled=True)


def pack_kernel(ix_ref, tok_ref, flag_ref, master_ref, one_ref, two_ref, out_ref):
    tok = tok_ref[...]
    flag = flag_ref[...]
    master = master_ref[...]
    high = master.astype(bf16).astype(f32)
    parts = (high, master - high, one_ref[...], two_ref[...])
    for x in range(NX):
        for y in range(NY):
            c = (y * NX + x) * 160
            d = x * NY + y
            out_ref[d, 0:32, :] = tok
            main = [p[:, c : c + LANES] for p in parts]
            rest = jnp.concatenate([p[:, c + LANES : c + 160] for p in parts], axis=1)
            out_ref[d, 32:48, :] = jnp.concatenate(main[:2], axis=0).astype(bf16)
            out_ref[d, 48:64, :] = jnp.concatenate(main[2:], axis=0).astype(bf16)
            out_ref[d, 64:80, :] = jnp.concatenate([rest, flag], axis=0).astype(bf16)


def pack(ix, tok, flag, master, one, two):
    rows = master.shape[0] // NX
    part = pl.BlockSpec((rows, master.shape[1]), lambda i, ix: (ix[0], 0))
    whole = lambda a: pl.BlockSpec(a.shape, lambda i, ix: (0, 0))
    return pl.pallas_call(
        pack_kernel,
        out_shape=jax.ShapeDtypeStruct((NX * NY, 80, LANES), bf16),
        grid_spec=pltpu.PrefetchScalarGridSpec(
            num_scalar_prefetch=1,
            grid=(1,),
            in_specs=[whole(tok), whole(flag), part, part, part],
            out_specs=pl.BlockSpec((NX * NY, 80, LANES), lambda i, ix: (0, 0, 0)),
        ),
        name="pack",
    )(ix, tok, flag, master, one, two)


def update(master, one, two, gradient, scale, fix):
    first = first_decay * one + (1.0 - first_decay) * gradient
    second = second_decay * two + (1.0 - second_decay) * gradient * gradient
    return master - scale * first / (jnp.sqrt(second * fix) + epsilon), first, second


def block_kernel(bucket_ref, scale_ref, fix_ref, first_ref, second_ref, grad_ref, part_ref, count_ref, params):
    tok = [first_ref[x * NY : (x + 1) * NY, 0:32, :].reshape(NY * 32, LANES) for x in range(NX)]
    og = [second_ref[x * NX : (x + 1) * NX, 0:40, :].reshape(160, LANES) for x in range(NX)]
    grad = jnp.zeros((NY * 32, 160), f32)
    for x in range(NX):
        grad += lax.dot_general(tok[x], og[x], (((1,), (1,)), ((), ())), preferred_element_type=f32)
    for y in range(NY):
        g = grad[y * 32 : (y + 1) * 32, :]
        tail = jnp.concatenate([g[8 * k : 8 * k + 8, LANES:160] for k in range(4)], axis=1)
        g = jnp.concatenate([g[:, :LANES], tail], axis=0).astype(bf16)
        for x in range(NX):
            grad_ref[x * NY + y] = g
    count = jnp.max(second_ref[:, 40:48, :].astype(f32), axis=0)
    count_ref[...] = count
    lane = lax.broadcasted_iota(jnp.int32, (8, LANES), 1)
    mine = jnp.max(jnp.where(lane == bucket_ref[0], count, 0.0), axis=(0, 1), keepdims=True)
    for x in range(NX):
        for y in range(NY):
            r = y * 32 + x * 8
            for k in range(2):
                two = first_ref[x * NY + y, 32 + 16 * k : 48 + 16 * k, :].astype(f32)
                params[2 * k, r : r + 8, :] = two[:8]
                params[2 * k + 1, r : r + 8, :] = two[8:]
            params[4, r : r + 8, :] = first_ref[x * NY + y, 64:80, :].astype(f32)[:8]
    scale, fix = scale_ref[bucket_ref[0]], fix_ref[bucket_ref[0]]
    halves = []
    for lo, hi in ((0, LANES), (LANES, 160)):
        if lo == 0:
            p = [params[k] for k in range(4)]
        else:
            rest = params[4]
            p = [rest[:, 32 * k : 32 * k + 32] for k in range(4)]
        old = p[0] + p[1]
        new, _, _ = update(old, p[2], p[3], grad[:, lo:hi], scale, fix)
        halves.append(jnp.where(mine == 0.0, new, old))
    weight = jnp.concatenate(halves, axis=1).T.astype(bf16)
    for x in range(NX):
        out = jnp.dot(weight, tok[x], preferred_element_type=f32)
        for k in range(NX):
            part_ref[x * NX + k] = out[40 * k : 40 * k + 40, :]


def block(bucket, scale, fix, first, second):
    smem, vmem = pl.BlockSpec(memory_space=SMEM), pl.BlockSpec(memory_space=VMEM)
    return pl.pallas_call(
        block_kernel,
        out_shape=(
            jax.ShapeDtypeStruct((NX * NY, 40, LANES), bf16),
            jax.ShapeDtypeStruct((NZC, 40, LANES), f32),
            jax.ShapeDtypeStruct((8, LANES), f32),
        ),
        in_specs=[smem, smem, smem, vmem, vmem],
        out_specs=(vmem, vmem, vmem),
        scratch_shapes=[pltpu.VMEM((5, NY * 32, LANES), f32)],
        name="block",
        compiler_params=SMALL,
    )(bucket, scale, fix, first, second)


def adam_kernel(grad_ref, row_ref, master_ref, one_ref, two_ref, master_out, one_out, two_out, half_out):
    pieces = []
    for x in range(NX):
        g = grad_ref[x, 0].astype(f32)
        tail = g[32:40]
        pieces.append(g[:32])
        pieces.append(jnp.concatenate([tail[:, 32 * k : 32 * k + 32] for k in range(4)], axis=0))
    grad = jnp.concatenate(pieces, axis=1)
    commit = row_ref[0:1, :] == 0.0
    master, one, two = master_ref[...], one_ref[...], two_ref[...]
    new, first, second = update(master, one, two, grad, row_ref[1:2, :], row_ref[2:3, :])
    master = jnp.where(commit, new, master)
    master_out[...] = master
    half_out[...] = master.astype(bf16)
    one_out[...] = jnp.where(commit, first, one)
    two_out[...] = jnp.where(commit, second, two)


def adam(grad, row, master, one, two):
    rows, width = master.shape
    step = width // NY
    full = pl.BlockSpec((rows, step), lambda i: (0, i))
    return pl.pallas_call(
        adam_kernel,
        out_shape=(*[jax.ShapeDtypeStruct(master.shape, f32)] * 3, jax.ShapeDtypeStruct(master.shape, bf16)),
        grid=(NY,),
        in_specs=[
            pl.BlockSpec((NX, 1, 40, LANES), lambda i: (0, i, 0, 0)),
            pl.BlockSpec((8, step), lambda i: (0, i)),
            full,
            full,
            full,
        ],
        out_specs=(full, full, full, full),
        name="adam",
        compiler_params=SMALL,
    )(grad.reshape(NX, NY, 40, LANES), row, master, one, two)


def local(tokens, out_grad, master, moment_one, moment_two, flags, steps, rate):
    rows, width = master.shape
    bucket_width = width // BUCKETS
    ix, iy = lax.axis_index("x"), lax.axis_index("y")

    times = (steps + 1).astype(f32)
    scales = rate[0] / (1.0 - jnp.power(f32(first_decay), times))
    fixes = 1.0 / (1.0 - jnp.power(f32(second_decay), times))
    bucket = ((iy * NX + ix) // 2)[None]

    mine = jnp.pad(flags.astype(f32), ((0, 7), (0, LANES - BUCKETS)))
    first = exchange(pack(ix[None], tokens.T, mine, master, moment_one, moment_two), XY)

    perm = [(zh * NX + x, x * NX + zh) for zh in range(NX) for x in range(NX)]
    og = lax.ppermute(out_grad.T, ("zh", "x"), perm)
    seen = jnp.max(first[:, 72:80, :], axis=0)
    og = jnp.concatenate([og, seen], axis=0)
    second = exchange(jnp.broadcast_to(og[None], (NZC, *og.shape)), ZC)

    grad, part, count = block(bucket, scales, fixes, first, second)
    total = jnp.sum(exchange(part, ZC), axis=0)
    result = lax.ppermute(total.astype(bf16), ("zh", "x"), perm).T
    grad = exchange(grad, XY)

    counts = count[0, :BUCKETS]
    row = jnp.stack([counts, scales, fixes, *[counts] * 5])
    row = jnp.repeat(row, bucket_width, axis=1)
    master_next, one_next, two_next, half = adam(grad, row, master, moment_one, moment_two)
    steps_next = steps + (counts == 0).astype(jnp.int32)
    return master_next, one_next, two_next, half, steps_next, result


def solution(mesh):
    split = Mesh(mesh.devices.reshape(8, 4, 2, 2, 4), ALL)
    in_specs = (P("x", FSDP), P("x", FSDP), P(FSDP), P(FSDP), P(FSDP), P(ALL), P(), P())
    out_specs = (P(FSDP), P(FSDP), P(FSDP), P(FSDP), P(), P("x", FSDP))
    return jax.shard_map(local, mesh=split, in_specs=in_specs, out_specs=out_specs, check_vma=False)
```

```python
import jax
import jax.numpy as jnp
from jax import lax
from jax.experimental import pallas as pl
from jax.experimental.pallas import tpu as pltpu
from jax.sharding import Mesh
from jax.sharding import PartitionSpec as P

BUCKETS = 16
FSDP = ("y", "zh", "zl", "c")
ALL = FSDP + ("x",)
ZC = ("zh", "zl", "c")
NX, NY, NZC = 4, 8, 16
LANES = 128
first_decay = 0.9
second_decay = 0.95
epsilon = 1e-08
bf16, f32 = jnp.bfloat16, jnp.float32
PART = bf16
VMEM, SMEM = pltpu.VMEM, pltpu.SMEM
SMALL = pltpu.CompilerParams(vmem_limit_bytes=16 * 1024 * 1024)


def exchange(x, axes):
    return lax.all_to_all(x, axes, 0, 0, tiled=True)


def pack_kernel(ix_ref, tok_ref, flag_ref, master_ref, one_ref, two_ref, out_ref):
    out_ref[0, 0:32, :] = tok_ref[...]
    flag = jnp.concatenate([flag_ref[...].astype(f32), jnp.zeros((1, LANES - BUCKETS), f32)], axis=1)
    out_ref[0, 192:200, :] = jnp.broadcast_to(flag, (8, LANES)).astype(bf16)
    for x in range(NX):

        @pl.when(ix_ref[0] == x)
        def _():
            c = x * 160
            master = master_ref[:, c : c + 160]
            high = master.astype(bf16).astype(f32)
            parts = (high, master - high, one_ref[:, c : c + 160], two_ref[:, c : c + 160])
            for k in range(4):
                out_ref[0, 32 + 32 * k : 64 + 32 * k, :] = parts[k][:, :LANES].astype(bf16)
            rest = jnp.concatenate([p[:, LANES:] for p in parts], axis=1)
            out_ref[0, 160:192, :] = rest.astype(bf16)


def pack(ix, tok, flag, master, one, two):
    rows, width = master.shape
    step = width // NY
    part = pl.BlockSpec((rows, step), lambda i, ix: (0, i))
    whole = lambda a: pl.BlockSpec(a.shape, lambda i, ix: (0, 0))
    return pl.pallas_call(
        pack_kernel,
        out_shape=jax.ShapeDtypeStruct((NY, 200, LANES), bf16),
        grid_spec=pltpu.PrefetchScalarGridSpec(
            num_scalar_prefetch=1,
            grid=(NY,),
            in_specs=[whole(tok), whole(flag), part, part, part],
            out_specs=pl.BlockSpec((1, 200, LANES), lambda i, ix: (i, 0, 0)),
        ),
        name="pack",
    )(ix, tok, flag, master, one, two)


def update(master, one, two, gradient, scale, fix):
    first = first_decay * one + (1.0 - first_decay) * gradient
    second = second_decay * two + (1.0 - second_decay) * gradient * gradient
    return master - scale * first / (jnp.sqrt(second * fix) + epsilon), first, second


def origin(ix, k):
    return lax.rem(ix + NX - k, NX)


def grad_kernel(ix_ref, t0, t1, t2, t3, second_ref, grad_ref, message_ref):
    grad = jnp.zeros((NY * 32, 160), f32)
    for k, t in enumerate((t0, t1, t2, t3)):
        og = second_ref[pl.ds(origin(ix_ref[0], k) * NX, NX), 0:40, :].reshape(160, LANES)
        grad += lax.dot_general(t[...], og, (((1,), (1,)), ((), ())), preferred_element_type=f32)
    grad_ref[...] = grad
    for y in range(NY):
        g = grad[y * 32 : (y + 1) * 32, :]
        tail = jnp.concatenate([g[8 * k : 8 * k + 8, LANES:160] for k in range(4)], axis=1)
        message_ref[y] = jnp.concatenate([g[:, :LANES], tail], axis=0).astype(bf16)


def gradient(ix, tok, second):
    smem, vmem = pl.BlockSpec(memory_space=SMEM), pl.BlockSpec(memory_space=VMEM)
    return pl.pallas_call(
        grad_kernel,
        out_shape=(
            jax.ShapeDtypeStruct((NY * 32, 160), f32),
            jax.ShapeDtypeStruct((NY, 40, LANES), bf16),
        ),
        in_specs=[smem, *[vmem] * 5],
        out_specs=(vmem, vmem),
        name="gradient",
        compiler_params=SMALL,
        cost_estimate=pl.CostEstimate(flops=2 * 256 * 160 * 512, bytes_accessed=1 << 20, transcendentals=0),
    )(ix, *tok, second)


def block_kernel(ix_ref, bucket_ref, scale_ref, fix_ref, grad_ref, t0, t1, t2, t3, first_ref, c0, c1, c2, c3, part_ref, count_ref):
    count = jnp.maximum(jnp.maximum(c0[...], c1[...]), jnp.maximum(c2[...], c3[...])).astype(f32)
    count_ref[...] = count
    lane = lax.broadcasted_iota(jnp.int32, (8, LANES), 1)
    mine = jnp.max(jnp.where(lane == bucket_ref[0], count, 0.0), axis=(0, 1), keepdims=True)
    scale, fix = scale_ref[bucket_ref[0]], fix_ref[bucket_ref[0]]
    rest = first_ref[:, 160:192, :].reshape(NY * 32, LANES).astype(f32)
    halves = []
    for lo, hi in ((0, LANES), (LANES, 160)):
        if lo == 0:
            p = [first_ref[:, 32 + 32 * k : 64 + 32 * k, :].reshape(NY * 32, LANES).astype(f32) for k in range(4)]
        else:
            p = [rest[:, 32 * k : 32 * k + 32] for k in range(4)]
        old = p[0] + p[1]
        new, _, _ = update(old, p[2], p[3], grad_ref[:, lo:hi], scale, fix)
        halves.append(jnp.where(mine == 0.0, new, old))
    weight = jnp.concatenate(halves, axis=1).T.astype(bf16)
    for k, t in enumerate((t0, t1, t2, t3)):
        out = jnp.dot(weight, t[...], preferred_element_type=f32).astype(part_ref.dtype)
        for j in range(NX):
            part_ref[origin(ix_ref[0], k) * NX + j] = out[40 * j : 40 * j + 40, :]


def block(ix, bucket, scales, fixes, grad, tok, first, count):
    smem, vmem = pl.BlockSpec(memory_space=SMEM), pl.BlockSpec(memory_space=VMEM)
    return pl.pallas_call(
        block_kernel,
        out_shape=(
            jax.ShapeDtypeStruct((NZC, 40, LANES), PART),
            jax.ShapeDtypeStruct((8, LANES), f32),
        ),
        in_specs=[smem] * 4 + [vmem] * 10,
        out_specs=(vmem, vmem),
        name="block",
        compiler_params=SMALL,
        cost_estimate=pl.CostEstimate(flops=2 * 256 * 160 * 512, bytes_accessed=1 << 20, transcendentals=1 << 16),
    )(ix, bucket, scales, fixes, grad, *tok, first, *count)


def adam_kernel(ix_ref, g0, g1, g2, g3, row_ref, master_ref, one_ref, two_ref, master_out, one_out, two_out, half_out, got):
    for k, g in enumerate((g0, g1, g2, g3)):
        got[origin(ix_ref[0], k)] = g[0]
    pieces = []
    for x in range(NX):
        g = got[x].astype(f32)
        tail = g[32:40]
        pieces.append(g[:32])
        pieces.append(jnp.concatenate([tail[:, 32 * k : 32 * k + 32] for k in range(4)], axis=0))
    grad = jnp.concatenate(pieces, axis=1)
    commit = row_ref[0:1, :] == 0.0
    master, one, two = master_ref[...], one_ref[...], two_ref[...]
    new, first, second = update(master, one, two, grad, row_ref[1:2, :], row_ref[2:3, :])
    master = jnp.where(commit, new, master)
    master_out[...] = master
    half_out[...] = master.astype(bf16)
    one_out[...] = jnp.where(commit, first, one)
    two_out[...] = jnp.where(commit, second, two)


def adam(ix, grads, row, master, one, two):
    rows, width = master.shape
    step = width // NY
    full = pl.BlockSpec((rows, step), lambda i: (0, i))
    piece = pl.BlockSpec((1, 40, LANES), lambda i: (i, 0, 0))
    return pl.pallas_call(
        adam_kernel,
        out_shape=(*[jax.ShapeDtypeStruct(master.shape, f32)] * 3, jax.ShapeDtypeStruct(master.shape, bf16)),
        grid=(NY,),
        in_specs=[
            pl.BlockSpec(memory_space=SMEM),
            *[piece] * NX,
            pl.BlockSpec((8, step), lambda i: (0, i)),
            full,
            full,
            full,
        ],
        out_specs=(full, full, full, full),
        scratch_shapes=[pltpu.VMEM((NX, 40, LANES), bf16)],
        name="adam",
        compiler_params=SMALL,
        cost_estimate=pl.CostEstimate(flops=1 << 23, bytes_accessed=5 << 20, transcendentals=1 << 18),
    )(ix, *grads, row, master, one, two)


def around(v):
    return [v] + [lax.ppermute(v, "x", [(i, (i + k) % NX) for i in range(NX)]) for k in range(1, NX)]


def local(tokens, out_grad, master, moment_one, moment_two, flags, steps, rate):
    rows, width = master.shape
    bucket_width = width // BUCKETS
    x, y = lax.axis_index("x"), lax.axis_index("y")
    ix, bucket = x[None], ((y * NX + x) // 2)[None]

    times = (steps + 1).astype(f32)
    scales = rate[0] / (1.0 - jnp.power(f32(first_decay), times))
    fixes = 1.0 / (1.0 - jnp.power(f32(second_decay), times))

    first = exchange(pack(ix, tokens.T, flags, master, moment_one, moment_two), "y")
    tok = around(first[:, :rows].reshape(NY * rows, LANES))

    perm = [(zh * NX + x, x * NX + zh) for zh in range(NX) for x in range(NX)]
    og = lax.ppermute(out_grad.T, ("zh", "x"), perm)
    seen = jnp.max(first[:, 192:200, :], axis=0)
    og = jnp.concatenate([og, seen], axis=0)
    second = exchange(jnp.broadcast_to(og[None], (NZC, *og.shape)), ZC)
    count = around(jnp.max(second[:, 40:48, :], axis=0))

    grad, message = gradient(ix, tok, second)
    grads = around(exchange(message, "y"))
    part, count = block(ix, bucket, scales, fixes, grad, tok, first, count)
    total = jnp.sum(exchange(part, ZC).astype(f32), axis=0)
    result = lax.ppermute(total.astype(bf16), ("zh", "x"), perm).T

    counts = count[0, :BUCKETS]
    row = jnp.stack([counts, scales, fixes, *[counts] * 5])
    row = jnp.repeat(row, bucket_width, axis=1)
    master_next, one_next, two_next, half = adam(ix, grads, row, master, moment_one, moment_two)
    steps_next = steps + (counts == 0).astype(jnp.int32)
    return master_next, one_next, two_next, half, steps_next, result


def solution(mesh):
    split = Mesh(mesh.devices.reshape(8, 4, 2, 2, 4), ALL)
    in_specs = (P("x", FSDP), P("x", FSDP), P(FSDP), P(FSDP), P(FSDP), P(ALL), P(), P())
    out_specs = (P(FSDP), P(FSDP), P(FSDP), P(FSDP), P(), P("x", FSDP))
    return jax.shard_map(local, mesh=split, in_specs=in_specs, out_specs=out_specs, check_vma=False)
```

```python
import jax
import jax.numpy as jnp
from jax import lax
from jax.experimental import pallas as pl
from jax.experimental.pallas import tpu as pltpu
from jax.sharding import Mesh
from jax.sharding import PartitionSpec as P

BUCKETS = 16
FSDP = ("y", "zh", "zl", "c")
ALL = FSDP + ("x",)
ZC = ("zh", "zl", "c")
XY = ("x", "y")
NX, NY, NZC = 4, 8, 16
LANES = 128
first_decay = 0.9
second_decay = 0.95
epsilon = 1e-08
bf16, f32 = jnp.bfloat16, jnp.float32
VMEM, SMEM = pltpu.VMEM, pltpu.SMEM
SMALL = pltpu.CompilerParams(vmem_limit_bytes=16 * 1024 * 1024)


def exchange(x, axes):
    return lax.all_to_all(x, axes, 0, 0, tiled=True)


def pack_kernel(ix_ref, tok_ref, flag_ref, master_ref, one_ref, two_ref, out_ref):
    flag = jnp.concatenate([flag_ref[...].astype(f32), jnp.zeros((1, LANES - BUCKETS), f32)], axis=1)
    flag = jnp.broadcast_to(flag, (8, LANES))
    tok = tok_ref[...]
    for x in range(NX):

        @pl.when(pl.program_id(0) == x)
        def _():
            for y in range(NY):
                c = (y * NX + x) * 160
                master = master_ref[:, c : c + 160]
                high = master.astype(bf16).astype(f32)
                parts = (high, master - high, one_ref[:, c : c + 160], two_ref[:, c : c + 160])
                main = [p[:, :LANES] for p in parts]
                rest = jnp.concatenate([p[:, LANES:] for p in parts], axis=1)
                out_ref[y, 0:32, :] = tok
                out_ref[y, 32:48, :] = jnp.concatenate(main[:2], axis=0).astype(bf16)
                out_ref[y, 48:64, :] = jnp.concatenate(main[2:], axis=0).astype(bf16)
                out_ref[y, 64:80, :] = jnp.concatenate([rest, flag], axis=0).astype(bf16)


def pack(ix, tok, flag, master, one, two):
    rows = master.shape[0] // NX
    part = pl.BlockSpec((rows, master.shape[1]), lambda i, ix: (ix[0], 0))
    whole = lambda a: pl.BlockSpec(a.shape, lambda i, ix: (0, 0))
    return pl.pallas_call(
        pack_kernel,
        out_shape=jax.ShapeDtypeStruct((NX * NY, 80, LANES), bf16),
        grid_spec=pltpu.PrefetchScalarGridSpec(
            num_scalar_prefetch=1,
            grid=(NX,),
            in_specs=[whole(tok), whole(flag), part, part, part],
            out_specs=pl.BlockSpec((NY, 80, LANES), lambda i, ix: (i, 0, 0)),
        ),
        name="pack",
    )(ix, tok, flag, master, one, two)


def update(master, one, two, gradient, scale, fix):
    first = first_decay * one + (1.0 - first_decay) * gradient
    second = second_decay * two + (1.0 - second_decay) * gradient * gradient
    return master - scale * first / (jnp.sqrt(second * fix) + epsilon), first, second


def block_kernel(bucket_ref, scale_ref, fix_ref, first_ref, second_ref, grad_ref, part_ref, count_ref, params):
    tok = [first_ref[x * NY : (x + 1) * NY, 0:32, :].reshape(NY * 32, LANES) for x in range(NX)]
    og = [second_ref[x * NX : (x + 1) * NX, 0:40, :].reshape(160, LANES) for x in range(NX)]
    grad = jnp.zeros((NY * 32, 160), f32)
    for x in range(NX):
        grad += lax.dot_general(tok[x], og[x], (((1,), (1,)), ((), ())), preferred_element_type=f32)
    for y in range(NY):
        g = grad[y * 32 : (y + 1) * 32, :]
        tail = jnp.concatenate([g[8 * k : 8 * k + 8, LANES:160] for k in range(4)], axis=1)
        g = jnp.concatenate([g[:, :LANES], tail], axis=0).astype(bf16)
        for x in range(NX):
            grad_ref[x * NY + y] = g
    count = jnp.max(second_ref[:, 40:48, :].astype(f32), axis=0)
    count_ref[...] = count
    lane = lax.broadcasted_iota(jnp.int32, (8, LANES), 1)
    mine = jnp.max(jnp.where(lane == bucket_ref[0], count, 0.0), axis=(0, 1), keepdims=True)
    for x in range(NX):
        for y in range(NY):
            r = y * 32 + x * 8
            for k in range(2):
                two = first_ref[x * NY + y, 32 + 16 * k : 48 + 16 * k, :].astype(f32)
                params[2 * k, r : r + 8, :] = two[:8]
                params[2 * k + 1, r : r + 8, :] = two[8:]
            params[4, r : r + 8, :] = first_ref[x * NY + y, 64:80, :].astype(f32)[:8]
    scale, fix = scale_ref[bucket_ref[0]], fix_ref[bucket_ref[0]]
    halves = []
    for lo, hi in ((0, LANES), (LANES, 160)):
        if lo == 0:
            p = [params[k] for k in range(4)]
        else:
            rest = params[4]
            p = [rest[:, 32 * k : 32 * k + 32] for k in range(4)]
        old = p[0] + p[1]
        new, _, _ = update(old, p[2], p[3], grad[:, lo:hi], scale, fix)
        halves.append(jnp.where(mine == 0.0, new, old))
    weight = jnp.concatenate(halves, axis=1).T.astype(bf16)
    for x in range(NX):
        out = jnp.dot(weight, tok[x], preferred_element_type=f32)
        for k in range(NX):
            part_ref[x * NX + k] = out[40 * k : 40 * k + 40, :].astype(bf16)


def block(bucket, scale, fix, first, second):
    smem, vmem = pl.BlockSpec(memory_space=SMEM), pl.BlockSpec(memory_space=VMEM)
    return pl.pallas_call(
        block_kernel,
        out_shape=(
            jax.ShapeDtypeStruct((NX * NY, 40, LANES), bf16),
            jax.ShapeDtypeStruct((NZC, 40, LANES), bf16),
            jax.ShapeDtypeStruct((8, LANES), f32),
        ),
        in_specs=[smem, smem, smem, vmem, vmem],
        out_specs=(vmem, vmem, vmem),
        scratch_shapes=[pltpu.VMEM((5, NY * 32, LANES), f32)],
        name="block",
        compiler_params=SMALL,
    )(bucket, scale, fix, first, second)


def adam_kernel(grad_ref, row_ref, result_ref, master_ref, one_ref, two_ref, master_out, one_out, two_out, half_out, result_out):
    step = master_out.shape[1]
    i = pl.program_id(0)
    here = pl.ds(pl.multiple_of(i * step, LANES), step)
    result_out[...] = result_ref[...]
    pieces = []
    for x in range(NX):
        g = grad_ref[x, i].astype(f32)
        tail = g[32:40]
        pieces.append(g[:32])
        pieces.append(jnp.concatenate([tail[:, 32 * k : 32 * k + 32] for k in range(4)], axis=0))
    grad = jnp.concatenate(pieces, axis=1)
    commit = row_ref[0:1, here] == 0.0
    master, one, two = master_ref[:, here], one_ref[:, here], two_ref[:, here]
    new, first, second = update(master, one, two, grad, row_ref[1:2, here], row_ref[2:3, here])
    master = jnp.where(commit, new, master)
    master_out[...] = master
    half_out[...] = master.astype(bf16)
    one_out[...] = jnp.where(commit, first, one)
    two_out[...] = jnp.where(commit, second, two)


def adam(grad, row, result, master, one, two):
    rows, width = master.shape
    step = width // NY
    full = pl.BlockSpec((rows, step), lambda i: (0, i))
    vmem = pl.BlockSpec(memory_space=VMEM)
    return pl.pallas_call(
        adam_kernel,
        out_shape=(
            *[jax.ShapeDtypeStruct(master.shape, f32)] * 3,
            jax.ShapeDtypeStruct(master.shape, bf16),
            jax.ShapeDtypeStruct(result.shape, bf16),
        ),
        grid=(NY,),
        in_specs=[vmem] * 6,
        out_specs=(full, full, full, full, pl.BlockSpec(result.shape, lambda i: (0, 0))),
        name="adam",
        compiler_params=SMALL,
    )(grad.reshape(NX, NY, 40, LANES), row, result, master, one, two)


def local(tokens, out_grad, master, moment_one, moment_two, flags, steps, rate):
    rows, width = master.shape
    bucket_width = width // BUCKETS
    ix, iy = lax.axis_index("x"), lax.axis_index("y")

    times = (steps + 1).astype(f32)
    scales = rate[0] / (1.0 - jnp.power(f32(first_decay), times))
    fixes = 1.0 / (1.0 - jnp.power(f32(second_decay), times))
    bucket = ((iy * NX + ix) // 2)[None]

    first = exchange(pack(ix[None], tokens.T, flags, master, moment_one, moment_two), XY)

    perm = [(zh * NX + x, x * NX + zh) for zh in range(NX) for x in range(NX)]
    og = lax.ppermute(out_grad.T, ("zh", "x"), perm)
    seen = jnp.max(first[:, 72:80, :], axis=0)
    og = jnp.concatenate([og, seen], axis=0)
    second = exchange(jnp.broadcast_to(og[None], (NZC, *og.shape)), ZC)

    grad, part, count = block(bucket, scales, fixes, first, second)
    total = jnp.sum(exchange(part, ZC).astype(f32), axis=0)
    result = lax.ppermute(total.astype(bf16), ("zh", "x"), perm)
    grad = exchange(grad, XY)

    counts = count[0, :BUCKETS]
    row = jnp.stack([counts, scales, fixes, *[counts] * 5])
    row = jnp.repeat(row, bucket_width, axis=1)
    master_next, one_next, two_next, half, result = adam(grad, row, result, master, moment_one, moment_two)
    steps_next = steps + (counts == 0).astype(jnp.int32)
    return master_next, one_next, two_next, half, steps_next, result.T


def solution(mesh):
    split = Mesh(mesh.devices.reshape(8, 4, 2, 2, 4), ALL)
    in_specs = (P("x", FSDP), P("x", FSDP), P(FSDP), P(FSDP), P(FSDP), P(ALL), P(), P())
    out_specs = (P(FSDP), P(FSDP), P(FSDP), P(FSDP), P(), P("x", FSDP))
    return jax.shard_map(local, mesh=split, in_specs=in_specs, out_specs=out_specs, check_vma=False)
```

```python
import jax
import jax.numpy as jnp
from jax import lax
from jax.experimental import pallas as pl
from jax.experimental.pallas import tpu as pltpu
from jax.sharding import Mesh
from jax.sharding import PartitionSpec as P

BUCKETS = 16
FSDP = ("y", "zh", "zl", "c")
ALL = FSDP + ("x",)
ZC = ("zh", "zl", "c")
XY = ("x", "y")
NX, NY, NZC = 4, 8, 16
STEPS = 4
LANES = 128
FLAGS = 96
first_decay = 0.9
second_decay = 0.95
epsilon = 1e-08
bf16, f32 = jnp.bfloat16, jnp.float32
VMEM, SMEM = pltpu.VMEM, pltpu.SMEM
SMALL = pltpu.CompilerParams(vmem_limit_bytes=16 * 1024 * 1024)


def exchange(x, axes):
    return lax.all_to_all(x, axes, 0, 0, tiled=True)


def pack_kernel(ix_ref, tok_ref, flag_ref, master_ref, one_ref, two_ref, out_ref):
    flag = jnp.concatenate([flag_ref[...].astype(f32), jnp.zeros((1, 32 - BUCKETS), f32)], axis=1)
    flag = jnp.broadcast_to(flag, (8, 32))
    tok = tok_ref[...]
    for x in range(NX):
        for y in range(NY):
            c = (y * NX + x) * 160
            d = x * NY + y
            parts = [p[:, c : c + 160] for p in (master_ref, one_ref, two_ref)]
            main = [p[:, :LANES] for p in parts]
            rest = jnp.concatenate([p[:, LANES:] for p in parts] + [flag], axis=1)
            out_ref[d, 0:32, :] = tok
            out_ref[d, 32:48, :] = jnp.concatenate(main[:2], axis=0).astype(bf16)
            out_ref[d, 48:64, :] = jnp.concatenate([main[2], rest], axis=0).astype(bf16)


def pack(ix, tok, flag, master, one, two):
    rows = master.shape[0] // NX
    part = pl.BlockSpec((rows, master.shape[1]), lambda i, ix: (ix[0], 0))
    whole = lambda a: pl.BlockSpec(a.shape, lambda i, ix: (0, 0))
    return pl.pallas_call(
        pack_kernel,
        out_shape=jax.ShapeDtypeStruct((NX * NY, 64, LANES), bf16),
        grid_spec=pltpu.PrefetchScalarGridSpec(
            num_scalar_prefetch=1,
            grid=(1,),
            in_specs=[whole(tok), whole(flag), part, part, part],
            out_specs=pl.BlockSpec((NX * NY, 64, LANES), lambda i, ix: (0, 0, 0)),
        ),
        name="pack",
    )(ix, tok, flag, master, one, two)


def update(master, one, two, gradient, scale, fix):
    first = first_decay * one + (1.0 - first_decay) * gradient
    second = second_decay * two + (1.0 - second_decay) * gradient * gradient
    return master - scale * first / (jnp.sqrt(second * fix) + epsilon), first, second


def block_kernel(bucket_ref, scale_ref, fix_ref, first_ref, second_ref, grad_ref, part_ref, count_ref, params):
    tok = [first_ref[x * NY : (x + 1) * NY, 0:32, :].reshape(NY * 32, LANES) for x in range(NX)]
    og = [second_ref[x * NX : (x + 1) * NX, 0:40, :].reshape(160, LANES) for x in range(NX)]
    grad = jnp.zeros((NY * 32, 160), f32)
    for x in range(NX):
        grad += lax.dot_general(tok[x], og[x], (((1,), (1,)), ((), ())), preferred_element_type=f32)
    for y in range(NY):
        g = grad[y * 32 : (y + 1) * 32, :]
        tail = jnp.concatenate([g[8 * k : 8 * k + 8, LANES:160] for k in range(4)], axis=1)
        g = jnp.concatenate([g[:, :LANES], tail], axis=0).astype(bf16)
        for x in range(NX):
            grad_ref[x * NY + y] = g
    count = jnp.max(second_ref[:, 40:48, :].astype(f32), axis=0)
    count_ref[...] = count
    lane = lax.broadcasted_iota(jnp.int32, (8, LANES), 1)
    mine = jnp.max(jnp.where(lane == FLAGS + bucket_ref[0], count, 0.0), axis=(0, 1), keepdims=True)
    for x in range(NX):
        for y in range(NY):
            r = y * 32 + x * 8
            for k in range(2):
                two = first_ref[x * NY + y, 32 + 16 * k : 48 + 16 * k, :].astype(f32)
                params[2 * k, r : r + 8, :] = two[:8]
                params[2 * k + 1, r : r + 8, :] = two[8:]
    scale, fix = scale_ref[bucket_ref[0]], fix_ref[bucket_ref[0]]
    halves = []
    for lo, hi in ((0, LANES), (LANES, 160)):
        if lo == 0:
            old, one, two = (params[k] for k in range(3))
        else:
            old, one, two = (params[3][:, 32 * k : 32 * k + 32] for k in range(3))
        new, _, _ = update(old, one, two, grad[:, lo:hi], scale, fix)
        halves.append(jnp.where(mine == 0.0, new, old))
    weight = jnp.concatenate(halves, axis=1).T.astype(bf16)
    for x in range(NX):
        out = jnp.dot(weight, tok[x], preferred_element_type=f32)
        for k in range(NX):
            part_ref[x * NX + k] = out[40 * k : 40 * k + 40, :].astype(bf16)


def block(bucket, scale, fix, first, second):
    smem, vmem = pl.BlockSpec(memory_space=SMEM), pl.BlockSpec(memory_space=VMEM)
    return pl.pallas_call(
        block_kernel,
        out_shape=(
            jax.ShapeDtypeStruct((NX * NY, 40, LANES), bf16),
            jax.ShapeDtypeStruct((NZC, 40, LANES), bf16),
            jax.ShapeDtypeStruct((8, LANES), f32),
        ),
        in_specs=[smem, smem, smem, vmem, vmem],
        out_specs=(vmem, vmem, vmem),
        scratch_shapes=[pltpu.VMEM((4, NY * 32, LANES), f32)],
        name="block",
        compiler_params=SMALL,
    )(bucket, scale, fix, first, second)


def adam_kernel(grad_ref, row_ref, result_ref, master_ref, one_ref, two_ref, master_out, one_out, two_out, half_out, result_out):
    step = master_out.shape[1]
    i = pl.program_id(0)
    here = pl.ds(pl.multiple_of(i * step, LANES), step)
    result_out[...] = result_ref[...]
    pieces = []
    for y in range(NY // STEPS):
        for x in range(NX):
            g = grad_ref[x, i * (NY // STEPS) + y].astype(f32)
            tail = g[32:40]
            pieces.append(g[:32])
            pieces.append(jnp.concatenate([tail[:, 32 * k : 32 * k + 32] for k in range(4)], axis=0))
    grad = jnp.concatenate(pieces, axis=1)
    commit = row_ref[0:1, here] == 0.0
    master, one, two = master_ref[:, here], one_ref[:, here], two_ref[:, here]
    new, first, second = update(master, one, two, grad, row_ref[1:2, here], row_ref[2:3, here])
    master = jnp.where(commit, new, master)
    master_out[...] = master
    half_out[...] = master.astype(bf16)
    one_out[...] = jnp.where(commit, first, one)
    two_out[...] = jnp.where(commit, second, two)


def adam(grad, row, result, master, one, two):
    rows, width = master.shape
    full = pl.BlockSpec((rows, width // STEPS), lambda i: (0, i))
    vmem = pl.BlockSpec(memory_space=VMEM)
    return pl.pallas_call(
        adam_kernel,
        out_shape=(
            *[jax.ShapeDtypeStruct(master.shape, f32)] * 3,
            jax.ShapeDtypeStruct(master.shape, bf16),
            jax.ShapeDtypeStruct(result.shape, bf16),
        ),
        grid=(STEPS,),
        in_specs=[vmem] * 6,
        out_specs=(full, full, full, full, pl.BlockSpec(result.shape, lambda i: (0, 0))),
        name="adam",
        compiler_params=SMALL,
    )(grad.reshape(NX, NY, 40, LANES), row, result, master, one, two)


def local(tokens, out_grad, master, moment_one, moment_two, flags, steps, rate):
    rows, width = master.shape
    bucket_width = width // BUCKETS
    ix, iy = lax.axis_index("x"), lax.axis_index("y")

    times = (steps + 1).astype(f32)
    scales = rate[0] / (1.0 - jnp.power(f32(first_decay), times))
    fixes = 1.0 / (1.0 - jnp.power(f32(second_decay), times))
    bucket = ((iy * NX + ix) // 2)[None]

    first = exchange(pack(ix[None], tokens.T, flags, master, moment_one, moment_two), XY)

    perm = [(zh * NX + x, x * NX + zh) for zh in range(NX) for x in range(NX)]
    og = lax.ppermute(out_grad.T, ("zh", "x"), perm)
    seen = jnp.max(first[:, 56:64, :], axis=0)
    og, scales, fixes, bucket = lax.optimization_barrier((jnp.concatenate([og, seen], axis=0), scales, fixes, bucket))
    second = exchange(jnp.broadcast_to(og[None], (NZC, *og.shape)), ZC)

    grad, part, count = block(bucket, scales, fixes, first, second)
    total = jnp.sum(exchange(part, ZC).astype(f32), axis=0)
    result = lax.ppermute(total.astype(bf16), ("zh", "x"), perm)
    grad = exchange(grad, XY)

    counts = count[0, FLAGS : FLAGS + BUCKETS]
    row = jnp.stack([counts, scales, fixes, *[counts] * 5])
    row = jnp.repeat(row, bucket_width, axis=1)
    master_next, one_next, two_next, half, result = adam(grad, row, result, master, moment_one, moment_two)
    steps_next = steps + (counts == 0).astype(jnp.int32)
    return master_next, one_next, two_next, half, steps_next, result.T


def solution(mesh):
    split = Mesh(mesh.devices.reshape(8, 4, 2, 2, 4), ALL)
    in_specs = (P("x", FSDP), P("x", FSDP), P(FSDP), P(FSDP), P(FSDP), P(ALL), P(), P())
    out_specs = (P(FSDP), P(FSDP), P(FSDP), P(FSDP), P(), P("x", FSDP))
    return jax.shard_map(local, mesh=split, in_specs=in_specs, out_specs=out_specs, check_vma=False)
```

```python
import jax
import jax.numpy as jnp
from jax import lax
from jax.experimental import pallas as pl
from jax.experimental.pallas import tpu as pltpu
from jax.sharding import Mesh
from jax.sharding import PartitionSpec as P

BUCKETS = 16
FSDP = ("y", "zh", "zl", "c")
ALL = FSDP + ("x",)
ZC = ("zh", "zl", "c")
XY = ("x", "y")
NX, NY, NZC = 4, 8, 16
STEPS = 4
LANES = 128
FLAGS = 96
first_decay = 0.9
second_decay = 0.95
epsilon = 1e-08
bf16, f32 = jnp.bfloat16, jnp.float32
VMEM, SMEM = pltpu.VMEM, pltpu.SMEM
SMALL = pltpu.CompilerParams(vmem_limit_bytes=16 * 1024 * 1024)


def exchange(x, axes):
    return lax.all_to_all(x, axes, 0, 0, tiled=True)


def pack_kernel(tok_hbm, flag_hbm, master_hbm, one_hbm, two_hbm, out_hbm, tok_ref, flag_ref, parts_ref, out_ref, sems, sent):
    mine = pl.ds(pl.multiple_of(lax.axis_index("x") * 8, 8), 8)
    reads = [
        pltpu.make_async_copy(tok_hbm, tok_ref, sems.at[0]),
        pltpu.make_async_copy(flag_hbm, flag_ref, sems.at[1]),
        *[
            pltpu.make_async_copy(ref.at[mine], parts_ref.at[k], sems.at[2 + k])
            for k, ref in enumerate((master_hbm, one_hbm, two_hbm))
        ],
    ]
    for read in reads:
        read.start()
    reads[0].wait()
    reads[1].wait()
    tok = tok_ref[...]
    for d in range(NX * NY):
        out_ref[d, 0:32, :] = tok
    flag = jnp.concatenate([flag_ref[...].astype(f32), jnp.zeros((1, 32 - BUCKETS), f32)], axis=1)
    flag = jnp.broadcast_to(flag, (8, 32))
    for read in reads[2:]:
        read.wait()
    writes = []
    for x in range(NX):
        for y in range(NY):
            c = (y * NX + x) * 160
            d = x * NY + y
            parts = [parts_ref[k, :, c : c + 160] for k in range(3)]
            main = [p[:, :LANES] for p in parts]
            rest = jnp.concatenate([p[:, LANES:] for p in parts] + [flag], axis=1)
            out_ref[d, 32:48, :] = jnp.concatenate(main[:2], axis=0).astype(bf16)
            out_ref[d, 48:64, :] = jnp.concatenate([main[2], rest], axis=0).astype(bf16)
        here = pl.ds(x * NY, NY)
        writes.append(pltpu.make_async_copy(out_ref.at[here], out_hbm.at[here], sent.at[x]))
        writes[-1].start()
    for write in writes:
        write.wait()


def pack(tok, flag, master, one, two):
    out = (NX * NY, 64, LANES)
    anywhere = pl.BlockSpec(memory_space=pl.ANY)
    return pl.pallas_call(
        pack_kernel,
        out_shape=jax.ShapeDtypeStruct(out, bf16),
        in_specs=[anywhere] * 5,
        out_specs=anywhere,
        scratch_shapes=[
            pltpu.VMEM(tok.shape, bf16),
            pltpu.VMEM(flag.shape, jnp.int32),
            pltpu.VMEM((3, 8, master.shape[1]), f32),
            pltpu.VMEM(out, bf16),
            pltpu.SemaphoreType.DMA((5,)),
            pltpu.SemaphoreType.DMA((NX,)),
        ],
        name="pack",
    )(tok, flag, master, one, two)


def update(master, one, two, gradient, scale, fix):
    first = first_decay * one + (1.0 - first_decay) * gradient
    second = second_decay * two + (1.0 - second_decay) * gradient * gradient
    return master - scale * first / (jnp.sqrt(second * fix) + epsilon), first, second


def block_kernel(bucket_ref, scale_ref, fix_ref, first_ref, second_ref, grad_hbm, part_ref, count_ref, message, sent):
    tok = [first_ref[x * NY : (x + 1) * NY, 0:32, :].reshape(NY * 32, LANES) for x in range(NX)]
    tok = jnp.concatenate(tok, axis=1)
    og = [second_ref[x * NX : (x + 1) * NX, 0:40, :].reshape(160, LANES) for x in range(NX)]
    og = jnp.concatenate(og, axis=1)
    grad = lax.dot_general(tok, og, (((1,), (1,)), ((), ())), preferred_element_type=f32)
    for y in range(NY):
        g = grad[y * 32 : (y + 1) * 32, :]
        tail = jnp.concatenate([g[8 * k : 8 * k + 8, LANES:160] for k in range(4)], axis=1)
        message[y] = jnp.concatenate([g[:, :LANES], tail], axis=0).astype(bf16)
    writes = [pltpu.make_async_copy(message, grad_hbm.at[pl.ds(x * NY, NY)], sent.at[x]) for x in range(NX)]
    for write in writes:
        write.start()
    count = jnp.max(second_ref[:, 40:48, :].astype(f32), axis=0)
    count_ref[...] = count
    lane = lax.broadcasted_iota(jnp.int32, (8, LANES), 1)
    mine = jnp.max(jnp.where(lane == FLAGS + bucket_ref[0], count, 0.0), axis=(0, 1), keepdims=True)
    order = [x * NY + y for y in range(NY) for x in range(NX)]
    pairs = [[first_ref[d, 32 + 16 * k : 48 + 16 * k, :].astype(f32) for d in order] for k in range(2)]
    params = [
        jnp.concatenate([p[8 * half : 8 * half + 8] for p in pairs[k]], axis=0) for k in range(2) for half in range(2)
    ]
    scale, fix = scale_ref[bucket_ref[0]], fix_ref[bucket_ref[0]]
    halves = []
    for lo, hi in ((0, LANES), (LANES, 160)):
        if lo == 0:
            old, one, two = params[:3]
        else:
            old, one, two = (params[3][:, 32 * k : 32 * k + 32] for k in range(3))
        new, _, _ = update(old, one, two, grad[:, lo:hi], scale, fix)
        halves.append(jnp.where(mine == 0.0, new, old))
    weight = jnp.concatenate(halves, axis=1).T.astype(bf16)
    out = jnp.dot(weight, tok, preferred_element_type=f32).astype(bf16)
    for x in range(NX):
        for k in range(NX):
            part_ref[x * NX + k] = out[40 * k : 40 * k + 40, x * LANES : (x + 1) * LANES]
    for write in writes:
        write.wait()


def block(bucket, scale, fix, first, second):
    smem, vmem = pl.BlockSpec(memory_space=SMEM), pl.BlockSpec(memory_space=VMEM)
    return pl.pallas_call(
        block_kernel,
        out_shape=(
            jax.ShapeDtypeStruct((NX * NY, 40, LANES), bf16),
            jax.ShapeDtypeStruct((NZC, 40, LANES), bf16),
            jax.ShapeDtypeStruct((8, LANES), f32),
        ),
        in_specs=[smem, smem, smem, vmem, vmem],
        out_specs=(pl.BlockSpec(memory_space=pl.ANY), vmem, vmem),
        scratch_shapes=[pltpu.VMEM((NY, 40, LANES), bf16), pltpu.SemaphoreType.DMA((NX,))],
        name="block",
        compiler_params=SMALL,
    )(bucket, scale, fix, first, second)


def adam_kernel(grad_ref, row_ref, result_ref, master_ref, one_ref, two_ref, master_out, one_out, two_out, half_out, result_out):
    step = master_out.shape[1]
    i = pl.program_id(0)
    here = pl.ds(pl.multiple_of(i * step, LANES), step)
    result_out[...] = result_ref[...]
    pieces = []
    for y in range(NY // STEPS):
        for x in range(NX):
            g = grad_ref[x, i * (NY // STEPS) + y].astype(f32)
            tail = g[32:40]
            pieces.append(g[:32])
            pieces.append(jnp.concatenate([tail[:, 32 * k : 32 * k + 32] for k in range(4)], axis=0))
    grad = jnp.concatenate(pieces, axis=1)
    commit = row_ref[0:1, here] == 0.0
    master, one, two = master_ref[:, here], one_ref[:, here], two_ref[:, here]
    new, first, second = update(master, one, two, grad, row_ref[1:2, here], row_ref[2:3, here])
    master = jnp.where(commit, new, master)
    master_out[...] = master
    half_out[...] = master.astype(bf16)
    one_out[...] = jnp.where(commit, first, one)
    two_out[...] = jnp.where(commit, second, two)


def adam(grad, row, result, master, one, two):
    rows, width = master.shape
    full = pl.BlockSpec((rows, width // STEPS), lambda i: (0, i))
    vmem = pl.BlockSpec(memory_space=VMEM)
    return pl.pallas_call(
        adam_kernel,
        out_shape=(
            *[jax.ShapeDtypeStruct(master.shape, f32)] * 3,
            jax.ShapeDtypeStruct(master.shape, bf16),
            jax.ShapeDtypeStruct(result.shape, bf16),
        ),
        grid=(STEPS,),
        in_specs=[vmem] * 6,
        out_specs=(full, full, full, full, pl.BlockSpec(result.shape, lambda i: (0, 0))),
        name="adam",
        compiler_params=SMALL,
    )(grad.reshape(NX, NY, 40, LANES), row, result, master, one, two)


def local(tokens, out_grad, master, moment_one, moment_two, flags, steps, rate):
    rows, width = master.shape
    bucket_width = width // BUCKETS
    ix, iy = lax.axis_index("x"), lax.axis_index("y")

    times = (steps + 1).astype(f32)
    scales = rate[0] / (1.0 - jnp.power(f32(first_decay), times))
    fixes = 1.0 / (1.0 - jnp.power(f32(second_decay), times))
    bucket = ((iy * NX + ix) // 2)[None]

    first = exchange(pack(tokens.T, flags, master, moment_one, moment_two), XY)

    perm = [(zh * NX + x, x * NX + zh) for zh in range(NX) for x in range(NX)]
    og = lax.ppermute(out_grad.T, ("zh", "x"), perm)
    seen = jnp.max(first[:, 56:64, :], axis=0)
    og, scales, fixes, bucket = lax.optimization_barrier((jnp.concatenate([og, seen], axis=0), scales, fixes, bucket))
    second = exchange(jnp.broadcast_to(og[None], (NZC, *og.shape)), ZC)

    grad, part, count = block(bucket, scales, fixes, first, second)
    total = jnp.sum(exchange(part, ZC).astype(f32), axis=0)
    result = lax.ppermute(total.astype(bf16), ("zh", "x"), perm)
    grad = exchange(grad, XY)

    counts = count[0, FLAGS : FLAGS + BUCKETS]
    row = jnp.stack([counts, scales, fixes, *[counts] * 5])
    row = jnp.repeat(row, bucket_width, axis=1)
    master_next, one_next, two_next, half, result = adam(grad, row, result, master, moment_one, moment_two)
    steps_next = steps + (counts == 0).astype(jnp.int32)
    return master_next, one_next, two_next, half, steps_next, result.T


def solution(mesh):
    split = Mesh(mesh.devices.reshape(8, 4, 2, 2, 4), ALL)
    in_specs = (P("x", FSDP), P("x", FSDP), P(FSDP), P(FSDP), P(FSDP), P(ALL), P(), P())
    out_specs = (P(FSDP), P(FSDP), P(FSDP), P(FSDP), P(), P("x", FSDP))
    return jax.shard_map(local, mesh=split, in_specs=in_specs, out_specs=out_specs, check_vma=False)
```

```python
import jax
import jax.numpy as jnp
from jax import lax
from jax.experimental import pallas as pl
from jax.experimental.pallas import tpu as pltpu
from jax.sharding import Mesh
from jax.sharding import PartitionSpec as P

BUCKETS = 16
FSDP = ("y", "zh", "zl", "c")
ALL = FSDP + ("x",)
ZC = ("zh", "zl", "c")
XY = ("x", "y")
NX, NY, NZC = 4, 8, 16
STEPS = 2
LANES = 128
FLAGS = 96
first_decay = 0.9
second_decay = 0.95
epsilon = 1e-08
bf16, f32 = jnp.bfloat16, jnp.float32
VMEM, SMEM = pltpu.VMEM, pltpu.SMEM
SMALL = pltpu.CompilerParams(vmem_limit_bytes=16 * 1024 * 1024)


def exchange(x, axes):
    return lax.all_to_all(x, axes, 0, 0, tiled=True)


def pack_kernel(tok_hbm, flag_hbm, master_hbm, one_hbm, two_hbm, out_hbm, tok_ref, flag_ref, parts_ref, out_ref, sems, sent):
    mine = pl.ds(pl.multiple_of(lax.axis_index("x") * 8, 8), 8)
    reads = [
        pltpu.make_async_copy(tok_hbm, tok_ref, sems.at[0]),
        pltpu.make_async_copy(flag_hbm, flag_ref, sems.at[1]),
        *[
            pltpu.make_async_copy(ref.at[mine], parts_ref.at[k], sems.at[2 + k])
            for k, ref in enumerate((master_hbm, one_hbm, two_hbm))
        ],
    ]
    for read in reads:
        read.start()
    reads[0].wait()
    reads[1].wait()
    tok = tok_ref[...]
    for d in range(NX * NY):
        out_ref[d, 0:32, :] = tok
    flag = jnp.concatenate([flag_ref[...].astype(f32), jnp.zeros((1, 32 - BUCKETS), f32)], axis=1)
    flag = jnp.broadcast_to(flag, (8, 32))
    for read in reads[2:]:
        read.wait()
    writes = []
    for x in range(NX):
        for y in range(NY):
            c = (y * NX + x) * 160
            d = x * NY + y
            parts = [parts_ref[k, :, c : c + 160] for k in range(3)]
            main = [p[:, :LANES] for p in parts]
            rest = jnp.concatenate([p[:, LANES:] for p in parts] + [flag], axis=1)
            out_ref[d, 32:48, :] = jnp.concatenate(main[:2], axis=0).astype(bf16)
            out_ref[d, 48:64, :] = jnp.concatenate([main[2], rest], axis=0).astype(bf16)
        here = pl.ds(x * NY, NY)
        writes.append(pltpu.make_async_copy(out_ref.at[here], out_hbm.at[here], sent.at[x]))
        writes[-1].start()
    for write in writes:
        write.wait()


def pack(tok, flag, master, one, two):
    out = (NX * NY, 64, LANES)
    anywhere = pl.BlockSpec(memory_space=pl.ANY)
    return pl.pallas_call(
        pack_kernel,
        out_shape=jax.ShapeDtypeStruct(out, bf16),
        in_specs=[anywhere] * 5,
        out_specs=anywhere,
        scratch_shapes=[
            pltpu.VMEM(tok.shape, bf16),
            pltpu.VMEM(flag.shape, jnp.int32),
            pltpu.VMEM((3, 8, master.shape[1]), f32),
            pltpu.VMEM(out, bf16),
            pltpu.SemaphoreType.DMA((5,)),
            pltpu.SemaphoreType.DMA((NX,)),
        ],
        name="pack",
    )(tok, flag, master, one, two)


def update(master, one, two, gradient, scale, fix):
    first = first_decay * one + (1.0 - first_decay) * gradient
    second = second_decay * two + (1.0 - second_decay) * gradient * gradient
    return master - scale * first / (jnp.sqrt(second * fix) + epsilon), first, second


def block_kernel(row_ref, first_ref, second_ref, grad_hbm, part_ref, count_ref, message, sent):
    tok = [first_ref[x * NY : (x + 1) * NY, 0:32, :].reshape(NY * 32, LANES) for x in range(NX)]
    tok = jnp.concatenate(tok, axis=1)
    og = [second_ref[x * NX : (x + 1) * NX, 0:40, :].reshape(160, LANES) for x in range(NX)]
    og = jnp.concatenate(og, axis=1)
    grad = lax.dot_general(tok, og, (((1,), (1,)), ((), ())), preferred_element_type=f32)
    for y in range(NY):
        g = grad[y * 32 : (y + 1) * 32, :]
        tail = jnp.concatenate([g[8 * k : 8 * k + 8, LANES:160] for k in range(4)], axis=1)
        message[y] = jnp.concatenate([g[:, :LANES], tail], axis=0).astype(bf16)
    writes = [pltpu.make_async_copy(message, grad_hbm.at[pl.ds(x * NY, NY)], sent.at[x]) for x in range(NX)]
    for write in writes:
        write.start()
    count = jnp.max(second_ref[:, 40:48, :].astype(f32), axis=0)
    count_ref[...] = count
    lane = lax.broadcasted_iota(jnp.int32, (8, LANES), 1)
    bucket = FLAGS + lax.div(lax.axis_index("y") * NX + lax.axis_index("x"), 2)
    pick = lambda v: jnp.max(jnp.where(lane == bucket, v, 0.0), axis=(0, 1), keepdims=True)
    mine, scale, fix = pick(count), pick(jnp.broadcast_to(row_ref[0:1, :], (8, LANES))), pick(jnp.broadcast_to(row_ref[1:2, :], (8, LANES)))
    order = [x * NY + y for y in range(NY) for x in range(NX)]
    pairs = [[first_ref[d, 32 + 16 * k : 48 + 16 * k, :].astype(f32) for d in order] for k in range(2)]
    params = [
        jnp.concatenate([p[8 * half : 8 * half + 8] for p in pairs[k]], axis=0) for k in range(2) for half in range(2)
    ]
    halves = []
    for lo, hi in ((0, LANES), (LANES, 160)):
        if lo == 0:
            old, one, two = params[:3]
        else:
            old, one, two = (params[3][:, 32 * k : 32 * k + 32] for k in range(3))
        new, _, _ = update(old, one, two, grad[:, lo:hi], scale, fix)
        halves.append(jnp.where(mine == 0.0, new, old))
    weight = jnp.concatenate(halves, axis=1).T.astype(bf16)
    out = jnp.dot(weight, tok, preferred_element_type=f32).astype(bf16)
    for x in range(NX):
        for k in range(NX):
            part_ref[x * NX + k] = out[40 * k : 40 * k + 40, x * LANES : (x + 1) * LANES]
    for write in writes:
        write.wait()


def block(row, first, second):
    vmem = pl.BlockSpec(memory_space=VMEM)
    return pl.pallas_call(
        block_kernel,
        out_shape=(
            jax.ShapeDtypeStruct((NX * NY, 40, LANES), bf16),
            jax.ShapeDtypeStruct((NZC, 40, LANES), bf16),
            jax.ShapeDtypeStruct((8, LANES), f32),
        ),
        in_specs=[vmem, vmem, vmem],
        out_specs=(pl.BlockSpec(memory_space=pl.ANY), vmem, vmem),
        scratch_shapes=[pltpu.VMEM((NY, 40, LANES), bf16), pltpu.SemaphoreType.DMA((NX,))],
        name="block",
        compiler_params=SMALL,
    )(row, first, second)


def adam_kernel(grad_ref, row_ref, result_ref, master_ref, one_ref, two_ref, master_out, one_out, two_out, half_out, result_out):
    step = master_out.shape[1]
    i = pl.program_id(0)
    here = pl.ds(pl.multiple_of(i * step, LANES), step)
    result_out[...] = result_ref[...]
    pieces = []
    for y in range(NY // STEPS):
        for x in range(NX):
            g = grad_ref[x, i * (NY // STEPS) + y].astype(f32)
            tail = g[32:40]
            pieces.append(g[:32])
            pieces.append(jnp.concatenate([tail[:, 32 * k : 32 * k + 32] for k in range(4)], axis=0))
    grad = jnp.concatenate(pieces, axis=1)
    commit = row_ref[0:1, here] == 0.0
    master, one, two = master_ref[:, here], one_ref[:, here], two_ref[:, here]
    new, first, second = update(master, one, two, grad, row_ref[1:2, here], row_ref[2:3, here])
    master = jnp.where(commit, new, master)
    master_out[...] = master
    half_out[...] = master.astype(bf16)
    one_out[...] = jnp.where(commit, first, one)
    two_out[...] = jnp.where(commit, second, two)


def adam(grad, row, result, master, one, two):
    rows, width = master.shape
    full = pl.BlockSpec((rows, width // STEPS), lambda i: (0, i))
    vmem = pl.BlockSpec(memory_space=VMEM)
    return pl.pallas_call(
        adam_kernel,
        out_shape=(
            *[jax.ShapeDtypeStruct(master.shape, f32)] * 3,
            jax.ShapeDtypeStruct(master.shape, bf16),
            jax.ShapeDtypeStruct(result.shape, bf16),
        ),
        grid=(STEPS,),
        in_specs=[vmem] * 6,
        out_specs=(full, full, full, full, pl.BlockSpec(result.shape, lambda i: (0, 0))),
        name="adam",
        compiler_params=SMALL,
    )(grad.reshape(NX, NY, 40, LANES), row, result, master, one, two)


def local(tokens, out_grad, master, moment_one, moment_two, flags, steps, rate):
    rows, width = master.shape
    bucket_width = width // BUCKETS

    times = (steps + 1).astype(f32)
    scales = rate[0] / (1.0 - jnp.power(f32(first_decay), times))
    fixes = 1.0 / (1.0 - jnp.power(f32(second_decay), times))
    own = jnp.pad(jnp.stack([scales, fixes]), ((0, 6), (FLAGS, LANES - FLAGS - BUCKETS)))

    first = exchange(pack(tokens.T, flags, master, moment_one, moment_two), XY)

    perm = [(zh * NX + x, x * NX + zh) for zh in range(NX) for x in range(NX)]
    og = lax.ppermute(out_grad.T, ("zh", "x"), perm)
    seen = jnp.max(first[:, 56:64, :], axis=0)
    og, scales, fixes, own = lax.optimization_barrier((jnp.concatenate([og, seen], axis=0), scales, fixes, own))
    second = exchange(jnp.broadcast_to(og[None], (NZC, *og.shape)), ZC)

    grad, part, count = block(own, first, second)
    total = jnp.sum(exchange(part, ZC).astype(f32), axis=0)
    result = lax.ppermute(total.astype(bf16), ("zh", "x"), perm)
    grad = exchange(grad, XY)

    counts = count[0, FLAGS : FLAGS + BUCKETS]
    row = jnp.stack([counts, scales, fixes, *[counts] * 5])
    row = jnp.repeat(row, bucket_width, axis=1)
    master_next, one_next, two_next, half, result = adam(grad, row, result, master, moment_one, moment_two)
    steps_next = steps + (counts == 0).astype(jnp.int32)
    return master_next, one_next, two_next, half, steps_next, result.T


def solution(mesh):
    split = Mesh(mesh.devices.reshape(8, 4, 2, 2, 4), ALL)
    in_specs = (P("x", FSDP), P("x", FSDP), P(FSDP), P(FSDP), P(FSDP), P(ALL), P(), P())
    out_specs = (P(FSDP), P(FSDP), P(FSDP), P(FSDP), P(), P("x", FSDP))
    return jax.shard_map(local, mesh=split, in_specs=in_specs, out_specs=out_specs, check_vma=False)
```

```python
import jax
import jax.numpy as jnp
from jax import lax
from jax.experimental import pallas as pl
from jax.experimental.pallas import tpu as pltpu
from jax.sharding import Mesh
from jax.sharding import PartitionSpec as P

BUCKETS = 16
FSDP = ("yq", "yp", "zq", "zp", "c")
ALL = FSDP + ("x",)
NEAR = ("x", "yp", "zp", "c")
FAR = ("yq", "zq")
NX, NE, NFAR = 4, 8, 16
STEPS = 2
LANES = 128
FLAGS = 96
first_decay = 0.9
second_decay = 0.95
epsilon = 1e-08
bf16, f32 = jnp.bfloat16, jnp.float32
VMEM = pltpu.VMEM
SMALL = pltpu.CompilerParams(vmem_limit_bytes=16 * 1024 * 1024)


def runs(x, e):
    yp, zc = e // 4, e % 4
    return [(2 * x + yp) * 640 + 160 * k + 40 * zc for k in range(4)]


def exchange(x, axes):
    return lax.all_to_all(x, axes, 0, 0, tiled=True)


def pack_kernel(tok_hbm, flag_hbm, master_hbm, one_hbm, two_hbm, out_hbm, tok_ref, flag_ref, parts_ref, out_ref, sems, sent):
    mine = pl.ds(pl.multiple_of(lax.axis_index("x") * 8, 8), 8)
    reads = [
        pltpu.make_async_copy(tok_hbm, tok_ref, sems.at[0]),
        pltpu.make_async_copy(flag_hbm, flag_ref, sems.at[1]),
        *[
            pltpu.make_async_copy(ref.at[mine], parts_ref.at[k], sems.at[2 + k])
            for k, ref in enumerate((master_hbm, one_hbm, two_hbm))
        ],
    ]
    for read in reads:
        read.start()
    reads[0].wait()
    reads[1].wait()
    tok = tok_ref[...]
    for d in range(NX * NE):
        out_ref[d, 0:32, :] = tok
    flag = jnp.concatenate([flag_ref[...].astype(f32), jnp.zeros((1, 32 - BUCKETS), f32)], axis=1)
    flag = jnp.broadcast_to(flag, (8, 32))
    for read in reads[2:]:
        read.wait()
    writes = []
    for x in range(NX):
        for e in range(NE):
            d = x * NE + e
            parts = [
                jnp.concatenate([parts_ref[k, :, c : c + 40] for c in runs(x, e)], axis=1) for k in range(3)
            ]
            main = [p[:, :LANES] for p in parts]
            rest = jnp.concatenate([p[:, LANES:] for p in parts] + [flag], axis=1)
            out_ref[d, 32:48, :] = jnp.concatenate(main[:2], axis=0).astype(bf16)
            out_ref[d, 48:64, :] = jnp.concatenate([main[2], rest], axis=0).astype(bf16)
        here = pl.ds(x * NE, NE)
        writes.append(pltpu.make_async_copy(out_ref.at[here], out_hbm.at[here], sent.at[x]))
        writes[-1].start()
    for write in writes:
        write.wait()


def pack(tok, flag, master, one, two):
    out = (NX * NE, 64, LANES)
    anywhere = pl.BlockSpec(memory_space=pl.ANY)
    return pl.pallas_call(
        pack_kernel,
        out_shape=jax.ShapeDtypeStruct(out, bf16),
        in_specs=[anywhere] * 5,
        out_specs=anywhere,
        scratch_shapes=[
            pltpu.VMEM(tok.shape, bf16),
            pltpu.VMEM(flag.shape, jnp.int32),
            pltpu.VMEM((3, 8, master.shape[1]), f32),
            pltpu.VMEM(out, bf16),
            pltpu.SemaphoreType.DMA((5,)),
            pltpu.SemaphoreType.DMA((NX,)),
        ],
        name="pack",
    )(tok, flag, master, one, two)


def update(master, one, two, gradient, scale, fix):
    first = first_decay * one + (1.0 - first_decay) * gradient
    second = second_decay * two + (1.0 - second_decay) * gradient * gradient
    return master - scale * first / (jnp.sqrt(second * fix) + epsilon), first, second


def block_kernel(row_ref, first_ref, second_ref, grad_hbm, part_ref, count_ref, message, sent):
    tok = [first_ref[x * NE : (x + 1) * NE, 0:32, :].reshape(NE * 32, LANES) for x in range(NX)]
    tok = jnp.concatenate(tok, axis=1)
    og = [second_ref[x * NX : (x + 1) * NX, 0:40, :].reshape(160, LANES) for x in range(NX)]
    og = jnp.concatenate(og, axis=1)
    grad = lax.dot_general(tok, og, (((1,), (1,)), ((), ())), preferred_element_type=f32)
    for y in range(NE):
        g = grad[y * 32 : (y + 1) * 32, :]
        tail = jnp.concatenate([g[8 * k : 8 * k + 8, LANES:160] for k in range(4)], axis=1)
        message[y] = jnp.concatenate([g[:, :LANES], tail], axis=0).astype(bf16)
    writes = [pltpu.make_async_copy(message, grad_hbm.at[pl.ds(x * NE, NE)], sent.at[x]) for x in range(NX)]
    for write in writes:
        write.start()
    count = jnp.max(second_ref[:, 40:48, :].astype(f32), axis=0)
    count_ref[...] = count
    lane = lax.broadcasted_iota(jnp.int32, (8, LANES), 1)
    bucket = FLAGS + 4 * lax.axis_index("x") + 2 * lax.axis_index("yp")
    table = [count, *[jnp.broadcast_to(row_ref[k : k + 1, :], (8, LANES)) for k in range(2)]]
    pick = lambda v, b: jnp.max(jnp.where(lane == b, v, 0.0), axis=(0, 1), keepdims=True)
    both = [[pick(v, bucket + k) for k in range(2)] for v in table]
    order = [x * NE + y for y in range(NE) for x in range(NX)]
    pairs = [[first_ref[d, 32 + 16 * k : 48 + 16 * k, :].astype(f32) for d in order] for k in range(2)]
    params = [
        jnp.concatenate([p[8 * half : 8 * half + 8] for p in pairs[k]], axis=0) for k in range(2) for half in range(2)
    ]
    halves = []
    for lo, hi in ((0, LANES), (LANES, 160)):
        if lo == 0:
            old, one, two = params[:3]
        else:
            old, one, two = (params[3][:, 32 * k : 32 * k + 32] for k in range(3))
        early = lax.broadcasted_iota(jnp.int32, (1, hi - lo), 1) + lo < 80
        mine, scale, fix = (jnp.where(early, *v) for v in both)
        new, _, _ = update(old, one, two, grad[:, lo:hi], scale, fix)
        halves.append(jnp.where(mine == 0.0, new, old))
    weight = jnp.concatenate(halves, axis=1).T.astype(bf16)
    out = jnp.dot(weight, tok, preferred_element_type=f32).astype(bf16)
    for x in range(NX):
        for k in range(NX):
            part_ref[x * NX + k] = out[40 * k : 40 * k + 40, x * LANES : (x + 1) * LANES]
    for write in writes:
        write.wait()


def block(row, first, second):
    vmem = pl.BlockSpec(memory_space=VMEM)
    return pl.pallas_call(
        block_kernel,
        out_shape=(
            jax.ShapeDtypeStruct((NX * NE, 40, LANES), bf16),
            jax.ShapeDtypeStruct((NFAR, 40, LANES), bf16),
            jax.ShapeDtypeStruct((8, LANES), f32),
        ),
        in_specs=[vmem, vmem, vmem],
        out_specs=(pl.BlockSpec(memory_space=pl.ANY), vmem, vmem),
        scratch_shapes=[pltpu.VMEM((NE, 40, LANES), bf16), pltpu.SemaphoreType.DMA((NX,))],
        name="block",
        compiler_params=SMALL,
    )(row, first, second)


def adam_kernel(grad_ref, row_ref, master_ref, one_ref, two_ref, master_out, one_out, two_out, half_out):
    step = master_out.shape[1]
    i = pl.program_id(0)
    here = pl.ds(pl.multiple_of(i * step, LANES), step)
    pieces = []
    for y in range(NE // STEPS):
        block = i * (NE // STEPS) + y
        got = []
        for zc in range(4):
            g = grad_ref[block * 4 + zc].astype(f32)
            tail = g[32:40]
            tail = jnp.concatenate([tail[:, 32 * k : 32 * k + 32] for k in range(4)], axis=0)
            got.append(jnp.concatenate([g[:32], tail], axis=1))
        pieces += [got[zc][:, 40 * k : 40 * k + 40] for k in range(4) for zc in range(4)]
    grad = jnp.concatenate(pieces, axis=1)
    commit = row_ref[0:1, here] == 0.0
    master, one, two = master_ref[:, here], one_ref[:, here], two_ref[:, here]
    new, first, second = update(master, one, two, grad, row_ref[1:2, here], row_ref[2:3, here])
    master = jnp.where(commit, new, master)
    master_out[...] = master
    half_out[...] = master.astype(bf16)
    one_out[...] = jnp.where(commit, first, one)
    two_out[...] = jnp.where(commit, second, two)


def adam(grad, row, master, one, two):
    rows, width = master.shape
    full = pl.BlockSpec((rows, width // STEPS), lambda i: (0, i))
    vmem = pl.BlockSpec(memory_space=VMEM)
    return pl.pallas_call(
        adam_kernel,
        out_shape=(
            *[jax.ShapeDtypeStruct(master.shape, f32)] * 3,
            jax.ShapeDtypeStruct(master.shape, bf16),
        ),
        grid=(STEPS,),
        in_specs=[vmem] * 5,
        out_specs=(full, full, full, full),
        name="adam",
        compiler_params=SMALL,
    )(grad, row, master, one, two)


def local(tokens, out_grad, master, moment_one, moment_two, flags, steps, rate):
    _, width = master.shape
    bucket_width = width // BUCKETS

    times = (steps + 1).astype(f32)
    scales = rate[0] / (1.0 - jnp.power(f32(first_decay), times))
    fixes = 1.0 / (1.0 - jnp.power(f32(second_decay), times))
    own = jnp.pad(jnp.stack([scales, fixes]), ((0, 6), (FLAGS, LANES - FLAGS - BUCKETS)))

    first = exchange(pack(tokens.T, flags, master, moment_one, moment_two), NEAR)

    perm = [(yq * NX + x, x * NX + yq) for yq in range(NX) for x in range(NX)]
    og = lax.ppermute(out_grad.T, ("yq", "x"), perm)
    seen = jnp.max(first[:, 56:64, :], axis=0)
    og, scales, fixes, own = lax.optimization_barrier((jnp.concatenate([og, seen], axis=0), scales, fixes, own))
    second = exchange(jnp.broadcast_to(og[None], (NFAR, *og.shape)), FAR)

    grad, part, count = block(own, first, second)
    total = jnp.sum(exchange(part, FAR).astype(f32), axis=0)
    result = lax.ppermute(total.astype(bf16), ("yq", "x"), perm)
    grad = exchange(grad, NEAR)

    counts = count[0, FLAGS : FLAGS + BUCKETS]
    row = jnp.stack([counts, scales, fixes, *[counts] * 5])
    row = jnp.repeat(row, bucket_width, axis=1)
    master_next, one_next, two_next, half = adam(grad, row, master, moment_one, moment_two)
    steps_next = steps + (counts == 0).astype(jnp.int32)
    return master_next, one_next, two_next, half, steps_next, result.T


def solution(mesh):
    split = Mesh(mesh.devices.reshape(4, 2, 4, 2, 2, 4), ALL)
    in_specs = (P("x", FSDP), P("x", FSDP), P(FSDP), P(FSDP), P(FSDP), P(ALL), P(), P())
    out_specs = (P(FSDP), P(FSDP), P(FSDP), P(FSDP), P(), P("x", FSDP))
    return jax.shard_map(local, mesh=split, in_specs=in_specs, out_specs=out_specs, check_vma=False)
```

```python
import jax
import jax.numpy as jnp
from jax import lax
from jax.experimental import pallas as pl
from jax.experimental.pallas import tpu as pltpu
from jax.sharding import Mesh
from jax.sharding import PartitionSpec as P

BUCKETS = 16
FSDP = ("yq", "yp", "zq", "zp", "c")
ALL = FSDP + ("x",)
NEAR = ("yp", "zp", "c", "x")
FAR = ("yq", "zq")
NX, NE, NFAR = 4, 8, 16
STEPS = 2
LANES = 128
FLAGS = 96
first_decay = 0.9
second_decay = 0.95
epsilon = 1e-08
bf16, f32 = jnp.bfloat16, jnp.float32
VMEM = pltpu.VMEM
SMALL = pltpu.CompilerParams(vmem_limit_bytes=16 * 1024 * 1024)


def runs(x, e):
    yp, zc = e // 4, e % 4
    return [(2 * x + yp) * 640 + 160 * k + 40 * zc for k in range(4)]


def exchange(x, axes):
    return lax.all_to_all(x, axes, 0, 0, tiled=True)


def pack_kernel(tok_hbm, flag_hbm, master_hbm, one_hbm, two_hbm, out_hbm, tok_ref, flag_ref, parts_ref, out_ref, sems, sent):
    mine = pl.ds(pl.multiple_of(lax.axis_index("x") * 8, 8), 8)
    reads = [
        pltpu.make_async_copy(tok_hbm, tok_ref, sems.at[0]),
        pltpu.make_async_copy(flag_hbm, flag_ref, sems.at[1]),
        *[
            pltpu.make_async_copy(ref.at[mine, pl.ds(x * 1280, 1280)], parts_ref.at[x, k], sems.at[2 + 3 * x + k])
            for x in range(NX)
            for k, ref in enumerate((master_hbm, one_hbm, two_hbm))
        ],
    ]
    for read in reads:
        read.start()
    reads[0].wait()
    reads[1].wait()
    tok = tok_ref[...]
    for x in range(NX):
        for e in range(NE):
            out_ref[e, x, 0:32, :] = tok
    flag = jnp.concatenate([flag_ref[...].astype(f32), jnp.zeros((1, 32 - BUCKETS), f32)], axis=1)
    flag = jnp.broadcast_to(flag, (8, 32))
    writes = []
    for x in range(NX):
        for read in reads[2 + 3 * x : 5 + 3 * x]:
            read.wait()
        for e in range(NE):
            first = [c - 1280 * x for c in runs(x, e)]
            parts = [
                jnp.concatenate([parts_ref[x, k, :, c : c + 40] for c in first], axis=1) for k in range(3)
            ]
            main = [p[:, :LANES] for p in parts]
            rest = jnp.concatenate([p[:, LANES:] for p in parts] + [flag], axis=1)
            out_ref[e, x, 32:48, :] = jnp.concatenate(main[:2], axis=0).astype(bf16)
            out_ref[e, x, 48:64, :] = jnp.concatenate([main[2], rest], axis=0).astype(bf16)
        writes.append(pltpu.make_async_copy(out_ref.at[:, x], out_hbm.at[:, x], sent.at[x]))
        writes[-1].start()
    for write in writes:
        write.wait()


def pack(tok, flag, master, one, two):
    out = (NE, NX, 64, LANES)
    anywhere = pl.BlockSpec(memory_space=pl.ANY)
    return pl.pallas_call(
        pack_kernel,
        out_shape=jax.ShapeDtypeStruct(out, bf16),
        in_specs=[anywhere] * 5,
        out_specs=anywhere,
        scratch_shapes=[
            pltpu.VMEM(tok.shape, bf16),
            pltpu.VMEM(flag.shape, jnp.int32),
            pltpu.VMEM((NX, 3, 8, master.shape[1] // NX), f32),
            pltpu.VMEM(out, bf16),
            pltpu.SemaphoreType.DMA((2 + 3 * NX,)),
            pltpu.SemaphoreType.DMA((NX,)),
        ],
        name="pack",
    )(tok, flag, master, one, two).reshape(NE * NX, 64, LANES)


def update(master, one, two, gradient, scale, fix):
    first = first_decay * one + (1.0 - first_decay) * gradient
    second = second_decay * two + (1.0 - second_decay) * gradient * gradient
    return master - scale * first / (jnp.sqrt(second * fix) + epsilon), first, second


def block_kernel(row_ref, first_ref, second_ref, grad_hbm, part_ref, count_ref, message, sent):
    tok = [jnp.concatenate([first_ref[e * NX + x, 0:32, :] for e in range(NE)], axis=0) for x in range(NX)]
    tok = jnp.concatenate(tok, axis=1)
    og = [second_ref[x * NX : (x + 1) * NX, 0:40, :].reshape(160, LANES) for x in range(NX)]
    og = jnp.concatenate(og, axis=1)
    grad = lax.dot_general(tok, og, (((1,), (1,)), ((), ())), preferred_element_type=f32)
    for y in range(NE):
        g = grad[y * 32 : (y + 1) * 32, :]
        tail = jnp.concatenate([g[8 * k : 8 * k + 8, LANES:160] for k in range(4)], axis=1)
        message[y] = jnp.concatenate([g[:, :LANES], tail], axis=0).astype(bf16)
    writes = [pltpu.make_async_copy(message, grad_hbm.at[:, x], sent.at[x]) for x in range(NX)]
    for write in writes:
        write.start()
    count = jnp.max(second_ref[:, 40:48, :].astype(f32), axis=0)
    count_ref[...] = count
    lane = lax.broadcasted_iota(jnp.int32, (8, LANES), 1)
    bucket = FLAGS + 4 * lax.axis_index("x") + 2 * lax.axis_index("yp")
    table = [count, *[jnp.broadcast_to(row_ref[k : k + 1, :], (8, LANES)) for k in range(2)]]
    pick = lambda v, b: jnp.max(jnp.where(lane == b, v, 0.0), axis=(0, 1), keepdims=True)
    both = [[pick(v, bucket + k) for k in range(2)] for v in table]
    order = range(NE * NX)
    pairs = [[first_ref[d, 32 + 16 * k : 48 + 16 * k, :].astype(f32) for d in order] for k in range(2)]
    params = [
        jnp.concatenate([p[8 * half : 8 * half + 8] for p in pairs[k]], axis=0) for k in range(2) for half in range(2)
    ]
    halves = []
    for lo, hi in ((0, LANES), (LANES, 160)):
        if lo == 0:
            old, one, two = params[:3]
        else:
            old, one, two = (params[3][:, 32 * k : 32 * k + 32] for k in range(3))
        early = lax.broadcasted_iota(jnp.int32, (1, hi - lo), 1) + lo < 80
        mine, scale, fix = (jnp.where(early, *v) for v in both)
        new, _, _ = update(old, one, two, grad[:, lo:hi], scale, fix)
        halves.append(jnp.where(mine == 0.0, new, old))
    weight = jnp.concatenate(halves, axis=1).T.astype(bf16)
    out = jnp.dot(weight, tok, preferred_element_type=f32).astype(bf16)
    for x in range(NX):
        for k in range(NX):
            part_ref[x * NX + k] = out[40 * k : 40 * k + 40, x * LANES : (x + 1) * LANES]
    for write in writes:
        write.wait()


def block(row, first, second):
    vmem = pl.BlockSpec(memory_space=VMEM)
    return pl.pallas_call(
        block_kernel,
        out_shape=(
            jax.ShapeDtypeStruct((NE, NX, 40, LANES), bf16),
            jax.ShapeDtypeStruct((NFAR, 40, LANES), bf16),
            jax.ShapeDtypeStruct((8, LANES), f32),
        ),
        in_specs=[vmem, vmem, vmem],
        out_specs=(pl.BlockSpec(memory_space=pl.ANY), vmem, vmem),
        scratch_shapes=[pltpu.VMEM((NE, 40, LANES), bf16), pltpu.SemaphoreType.DMA((NX,))],
        name="block",
        compiler_params=SMALL,
    )(row, first, second)


def adam_kernel(grad_ref, row_ref, master_ref, one_ref, two_ref, master_out, one_out, two_out, half_out):
    step = master_out.shape[1]
    i = pl.program_id(0)
    here = pl.ds(pl.multiple_of(i * step, LANES), step)
    pieces = []
    for y in range(NE // STEPS):
        x, yp = i * (NE // STEPS // 2) + y // 2, y % 2
        got = []
        for zc in range(4):
            g = grad_ref[(yp * 4 + zc) * NX + x].astype(f32)
            tail = g[32:40]
            tail = jnp.concatenate([tail[:, 32 * k : 32 * k + 32] for k in range(4)], axis=0)
            got.append(jnp.concatenate([g[:32], tail], axis=1))
        pieces += [got[zc][:, 40 * k : 40 * k + 40] for k in range(4) for zc in range(4)]
    grad = jnp.concatenate(pieces, axis=1)
    commit = row_ref[0:1, here] == 0.0
    master, one, two = master_ref[:, here], one_ref[:, here], two_ref[:, here]
    new, first, second = update(master, one, two, grad, row_ref[1:2, here], row_ref[2:3, here])
    master = jnp.where(commit, new, master)
    master_out[...] = master
    half_out[...] = master.astype(bf16)
    one_out[...] = jnp.where(commit, first, one)
    two_out[...] = jnp.where(commit, second, two)


def adam(grad, row, master, one, two):
    rows, width = master.shape
    full = pl.BlockSpec((rows, width // STEPS), lambda i: (0, i))
    vmem = pl.BlockSpec(memory_space=VMEM)
    return pl.pallas_call(
        adam_kernel,
        out_shape=(
            *[jax.ShapeDtypeStruct(master.shape, f32)] * 3,
            jax.ShapeDtypeStruct(master.shape, bf16),
        ),
        grid=(STEPS,),
        in_specs=[vmem] * 5,
        out_specs=(full, full, full, full),
        name="adam",
        compiler_params=SMALL,
    )(grad, row, master, one, two)


def local(tokens, out_grad, master, moment_one, moment_two, flags, steps, rate):
    _, width = master.shape
    bucket_width = width // BUCKETS

    times = (steps + 1).astype(f32)
    scales = rate[0] / (1.0 - jnp.power(f32(first_decay), times))
    fixes = 1.0 / (1.0 - jnp.power(f32(second_decay), times))
    own = jnp.pad(jnp.stack([scales, fixes]), ((0, 6), (FLAGS, LANES - FLAGS - BUCKETS)))

    first = exchange(pack(tokens.T, flags, master, moment_one, moment_two), NEAR)

    perm = [(yq * NX + x, x * NX + yq) for yq in range(NX) for x in range(NX)]
    og = lax.ppermute(out_grad.T, ("yq", "x"), perm)
    seen = jnp.max(first[:, 56:64, :], axis=0)
    og, scales, fixes, own = lax.optimization_barrier((jnp.concatenate([og, seen], axis=0), scales, fixes, own))
    second = exchange(jnp.broadcast_to(og[None], (NFAR, *og.shape)), FAR)

    grad, part, count = block(own, first, second)
    total = jnp.sum(exchange(part, FAR).astype(f32), axis=0)
    result = lax.ppermute(total.astype(bf16), ("yq", "x"), perm)
    grad = exchange(grad.reshape(NE * NX, 40, LANES), NEAR)

    counts = count[0, FLAGS : FLAGS + BUCKETS]
    row = jnp.stack([counts, scales, fixes, *[counts] * 5])
    row = jnp.repeat(row, bucket_width, axis=1)
    master_next, one_next, two_next, half = adam(grad, row, master, moment_one, moment_two)
    steps_next = steps + (counts == 0).astype(jnp.int32)
    return master_next, one_next, two_next, half, steps_next, result.T


def solution(mesh):
    split = Mesh(mesh.devices.reshape(4, 2, 4, 2, 2, 4), ALL)
    in_specs = (P("x", FSDP), P("x", FSDP), P(FSDP), P(FSDP), P(FSDP), P(ALL), P(), P())
    out_specs = (P(FSDP), P(FSDP), P(FSDP), P(FSDP), P(), P("x", FSDP))
    return jax.shard_map(local, mesh=split, in_specs=in_specs, out_specs=out_specs, check_vma=False)
```

```python
import jax
import jax.numpy as jnp
from jax import lax
from jax.experimental import pallas as pl
from jax.experimental.pallas import tpu as pltpu
from jax.sharding import Mesh
from jax.sharding import PartitionSpec as P

BUCKETS = 16
FSDP = ("yq", "yp", "zq", "zp", "c")
ALL = FSDP + ("x",)
NEAR = ("yp", "zp", "c", "x")
FAR = ("yq", "zq")
NX, NE, NFAR = 4, 8, 16
STEPS = 2
LANES = 128
FLAGS = 96
first_decay = 0.9
second_decay = 0.95
epsilon = 1e-08
bf16, f32 = jnp.bfloat16, jnp.float32
VMEM = pltpu.VMEM
SMALL = pltpu.CompilerParams(vmem_limit_bytes=16 * 1024 * 1024)


def runs(x, e):
    yp, zc = e // 4, e % 4
    return [(2 * x + yp) * 640 + 160 * k + 40 * zc for k in range(4)]


def across(x):
    return (x + 2) % NX


def exchange(x, axes):
    return lax.all_to_all(x, axes, 0, 0, tiled=True)


def pack_kernel(tok_hbm, flag_hbm, master_hbm, one_hbm, two_hbm, out_hbm, tok_ref, flag_ref, parts_ref, out_ref, sems, sent):
    mine = pl.ds(pl.multiple_of(lax.axis_index("x") * 8, 8), 8)
    reads = [
        pltpu.make_async_copy(tok_hbm, tok_ref, sems.at[0]),
        pltpu.make_async_copy(flag_hbm, flag_ref, sems.at[1]),
        *[
            pltpu.make_async_copy(ref.at[mine, pl.ds(x * 1280, 1280)], parts_ref.at[x, k], sems.at[2 + 3 * x + k])
            for x in range(NX)
            for k, ref in enumerate((master_hbm, one_hbm, two_hbm))
        ],
    ]
    for read in reads[2:5] + reads[:2] + reads[5:]:
        read.start()
    reads[0].wait()
    reads[1].wait()
    tok = tok_ref[...]
    for x in range(NX):
        for e in range(NE):
            out_ref[e, x, 0:32, :] = tok
    flag = jnp.concatenate([flag_ref[...].astype(f32), jnp.zeros((1, 32 - BUCKETS), f32)], axis=1)
    flag = jnp.broadcast_to(flag, (8, 32))
    writes = []
    for x in range(NX):
        for read in reads[2 + 3 * x : 5 + 3 * x]:
            read.wait()
        for e in range(NE):
            first = [c - 1280 * x for c in runs(x, e)]
            parts = [
                jnp.concatenate([parts_ref[x, k, :, c : c + 40] for c in first], axis=1) for k in range(3)
            ]
            main = [p[:, :LANES] for p in parts]
            rest = jnp.concatenate([p[:, LANES:] for p in parts] + [flag], axis=1)
            out_ref[e, x, 32:48, :] = jnp.concatenate(main[:2], axis=0).astype(bf16)
            out_ref[e, x, 48:64, :] = jnp.concatenate([main[2], rest], axis=0).astype(bf16)
        writes.append(pltpu.make_async_copy(out_ref.at[:, x], out_hbm.at[:, x], sent.at[x]))
        writes[-1].start()
    for write in writes:
        write.wait()


def pack(tok, flag, master, one, two):
    out = (NE, NX, 64, LANES)
    anywhere = pl.BlockSpec(memory_space=pl.ANY)
    return pl.pallas_call(
        pack_kernel,
        out_shape=jax.ShapeDtypeStruct(out, bf16),
        in_specs=[anywhere] * 5,
        out_specs=anywhere,
        scratch_shapes=[
            pltpu.VMEM(tok.shape, bf16),
            pltpu.VMEM(flag.shape, jnp.int32),
            pltpu.VMEM((NX, 3, 8, master.shape[1] // NX), f32),
            pltpu.VMEM(out, bf16),
            pltpu.SemaphoreType.DMA((2 + 3 * NX,)),
            pltpu.SemaphoreType.DMA((NX,)),
        ],
        name="pack",
    )(tok, flag, master, one, two).reshape(NE * NX, 64, LANES)


def update(master, one, two, gradient, scale, fix):
    first = first_decay * one + (1.0 - first_decay) * gradient
    second = second_decay * two + (1.0 - second_decay) * gradient * gradient
    return master - scale * first / (jnp.sqrt(second * fix) + epsilon), first, second


def block_kernel(row_ref, first_ref, second_ref, grad_hbm, part_ref, count_ref, message, sent):
    tok = [jnp.concatenate([first_ref[e * NX + x, 0:32, :] for e in range(NE)], axis=0) for x in range(NX)]
    tok = jnp.concatenate(tok, axis=1)
    og = [second_ref[q * NX : (q + 1) * NX, 0:40, :].reshape(160, LANES) for q in map(across, range(NX))]
    og = jnp.concatenate(og, axis=1)
    grad = lax.dot_general(tok, og, (((1,), (1,)), ((), ())), preferred_element_type=f32)
    for y in range(NE):
        g = grad[y * 32 : (y + 1) * 32, :]
        tail = jnp.concatenate([g[8 * k : 8 * k + 8, LANES:160] for k in range(4)], axis=1)
        message[y] = jnp.concatenate([g[:, :LANES], tail], axis=0).astype(bf16)
    writes = [pltpu.make_async_copy(message, grad_hbm.at[:, x], sent.at[x]) for x in range(NX)]
    for write in writes:
        write.start()
    count = jnp.max(second_ref[:, 40:48, :].astype(f32), axis=0)
    count_ref[...] = count
    lane = lax.broadcasted_iota(jnp.int32, (8, LANES), 1)
    bucket = FLAGS + 4 * lax.axis_index("x") + 2 * lax.axis_index("yp")
    table = [count, *[jnp.broadcast_to(row_ref[k : k + 1, :], (8, LANES)) for k in range(2)]]
    pick = lambda v, b: jnp.max(jnp.where(lane == b, v, 0.0), axis=(0, 1), keepdims=True)
    both = [[pick(v, bucket + k) for k in range(2)] for v in table]
    order = range(NE * NX)
    pairs = [[first_ref[d, 32 + 16 * k : 48 + 16 * k, :].astype(f32) for d in order] for k in range(2)]
    params = [
        jnp.concatenate([p[8 * half : 8 * half + 8] for p in pairs[k]], axis=0) for k in range(2) for half in range(2)
    ]
    halves = []
    for lo, hi in ((0, LANES), (LANES, 160)):
        if lo == 0:
            old, one, two = params[:3]
        else:
            old, one, two = (params[3][:, 32 * k : 32 * k + 32] for k in range(3))
        early = lax.broadcasted_iota(jnp.int32, (1, hi - lo), 1) + lo < 80
        mine, scale, fix = (jnp.where(early, *v) for v in both)
        new, _, _ = update(old, one, two, grad[:, lo:hi], scale, fix)
        halves.append(jnp.where(mine == 0.0, new, old))
    weight = jnp.concatenate(halves, axis=1).T.astype(bf16)
    out = jnp.dot(weight, tok, preferred_element_type=f32).astype(bf16)
    for x in range(NX):
        for k in range(NX):
            part_ref[across(x) * NX + k] = out[40 * k : 40 * k + 40, x * LANES : (x + 1) * LANES]
    for write in writes:
        write.wait()


def block(row, first, second):
    vmem = pl.BlockSpec(memory_space=VMEM)
    return pl.pallas_call(
        block_kernel,
        out_shape=(
            jax.ShapeDtypeStruct((NE, NX, 40, LANES), bf16),
            jax.ShapeDtypeStruct((NFAR, 40, LANES), bf16),
            jax.ShapeDtypeStruct((8, LANES), f32),
        ),
        in_specs=[vmem, vmem, vmem],
        out_specs=(pl.BlockSpec(memory_space=pl.ANY), vmem, vmem),
        scratch_shapes=[pltpu.VMEM((NE, 40, LANES), bf16), pltpu.SemaphoreType.DMA((NX,))],
        name="block",
        compiler_params=SMALL,
    )(row, first, second)


def adam_kernel(grad_ref, row_ref, master_ref, one_ref, two_ref, master_out, one_out, two_out, half_out):
    step = master_out.shape[1]
    i = pl.program_id(0)
    here = pl.ds(pl.multiple_of(i * step, LANES), step)
    pieces = []
    for y in range(NE // STEPS):
        x, yp = i * (NE // STEPS // 2) + y // 2, y % 2
        got = []
        for zc in range(4):
            g = grad_ref[(yp * 4 + zc) * NX + x].astype(f32)
            tail = g[32:40]
            tail = jnp.concatenate([tail[:, 32 * k : 32 * k + 32] for k in range(4)], axis=0)
            got.append(jnp.concatenate([g[:32], tail], axis=1))
        pieces += [got[zc][:, 40 * k : 40 * k + 40] for k in range(4) for zc in range(4)]
    grad = jnp.concatenate(pieces, axis=1)
    commit = row_ref[0:1, here] == 0.0
    master, one, two = master_ref[:, here], one_ref[:, here], two_ref[:, here]
    new, first, second = update(master, one, two, grad, row_ref[1:2, here], row_ref[2:3, here])
    master = jnp.where(commit, new, master)
    master_out[...] = master
    half_out[...] = master.astype(bf16)
    one_out[...] = jnp.where(commit, first, one)
    two_out[...] = jnp.where(commit, second, two)


def adam(grad, row, master, one, two):
    rows, width = master.shape
    full = pl.BlockSpec((rows, width // STEPS), lambda i: (0, i))
    vmem = pl.BlockSpec(memory_space=VMEM)
    return pl.pallas_call(
        adam_kernel,
        out_shape=(
            *[jax.ShapeDtypeStruct(master.shape, f32)] * 3,
            jax.ShapeDtypeStruct(master.shape, bf16),
        ),
        grid=(STEPS,),
        in_specs=[vmem] * 5,
        out_specs=(full, full, full, full),
        name="adam",
        compiler_params=SMALL,
    )(grad, row, master, one, two)


def local(tokens, out_grad, master, moment_one, moment_two, flags, steps, rate):
    _, width = master.shape
    bucket_width = width // BUCKETS

    times = (steps + 1).astype(f32)
    scales = rate[0] / (1.0 - jnp.power(f32(first_decay), times))
    fixes = 1.0 / (1.0 - jnp.power(f32(second_decay), times))
    own = jnp.pad(jnp.stack([scales, fixes]), ((0, 6), (FLAGS, LANES - FLAGS - BUCKETS)))

    first = exchange(pack(tokens.T, flags, master, moment_one, moment_two), NEAR)

    there = [(yq * NX + x, across(x) * NX + yq) for yq in range(NX) for x in range(NX)]
    back = [(b, a) for a, b in there]
    og = lax.ppermute(out_grad.T, ("yq", "x"), there)
    seen = jnp.max(first[:, 56:64, :], axis=0)
    og, scales, fixes, own = lax.optimization_barrier((jnp.concatenate([og, seen], axis=0), scales, fixes, own))
    second = exchange(jnp.broadcast_to(og[None], (NFAR, *og.shape)), FAR)

    grad, part, count = block(own, first, second)
    total = jnp.sum(exchange(part, FAR).astype(f32), axis=0)
    result = lax.ppermute(total.astype(bf16), ("yq", "x"), back)
    grad = exchange(grad.reshape(NE * NX, 40, LANES), NEAR)

    counts = count[0, FLAGS : FLAGS + BUCKETS]
    row = jnp.stack([counts, scales, fixes, *[counts] * 5])
    row = jnp.repeat(row, bucket_width, axis=1)
    master_next, one_next, two_next, half = adam(grad, row, master, moment_one, moment_two)
    steps_next = steps + (counts == 0).astype(jnp.int32)
    return master_next, one_next, two_next, half, steps_next, result.T


def solution(mesh):
    split = Mesh(mesh.devices.reshape(4, 2, 4, 2, 2, 4), ALL)
    in_specs = (P("x", FSDP), P("x", FSDP), P(FSDP), P(FSDP), P(FSDP), P(ALL), P(), P())
    out_specs = (P(FSDP), P(FSDP), P(FSDP), P(FSDP), P(), P("x", FSDP))
    return jax.shard_map(local, mesh=split, in_specs=in_specs, out_specs=out_specs, check_vma=False)
```
